128 devices in a mesh: row: 4 (over z), col: 16 (over x, y_hi, core), depth: 2 (over y_lo).
Axes of the slice: x: 4, y: 4 (y_hi: 2, y_lo: 2; y = y_hi * 2 + y_lo), z: 4, core: 2. Of those that a mesh axis runs over, the one named last changes fastest.
Arguments:
- tokens: bfloat16 [8192, 8192], P(('row', 'col'), 'depth'), may hold values from -0.15625 to 0.15625
- weight: bfloat16 [8192, 8192], P('depth', ('col', 'row')), may hold values from -0.0625 to 0.0625
- grad_output: bfloat16 [8192, 8192], P('row', ('col', 'depth')), may hold values from -6 to 6
Outputs:
- grad_input: bfloat16 [8192, 8192], P(('row', 'col'), 'depth')
- grad_weight: bfloat16 [8192, 8192], P('depth', ('col', 'row'))
The draws below stay inside these ranges and needn't reach their ends.
All inputs are finite; a program needn't handle non-finite values.
Results may differ from the reference program's by a relative error of at most 0.001.
Values may be sent and summed in bfloat16 or wider, within the bound.
A program may use at most 128 MiB of HBM per device.

```python
import jax
import jax.numpy as jnp

D_IN = 8192
D_OUT = 8192
TOKENS = 8192


def spiked(drawn, stream_key, source, target, parts, factor):
    def block_of(axis_at):
        return (jnp.arange(drawn.shape[axis_at]) // (drawn.shape[axis_at] // parts)).reshape((-1,) + (1,) * (drawn.ndim - 1 - axis_at))

    one_side = jax.random.permutation(stream_key, parts)[block_of(target)]
    other_side = (block_of(target) + parts // 2) % parts
    return jnp.where((block_of(source) == one_side) | (block_of(source) == other_side), factor * drawn, drawn)


def shard_levels(rng, extent, pieces, low, top_value):
    gain, own = 1.0, jax.random.fold_in(rng, 6)
    for position, shards_of in pieces:
        steps = jnp.exp(jax.random.uniform(jax.random.fold_in(own, position), (shards_of,), jnp.float32, low / len(pieces), top_value / len(pieces)))
        gain = gain * jnp.repeat(steps, extent[position] // shards_of).reshape([-1 if axis == position else 1 for axis in range(len(extent))])
    return gain


def bell_draw(rng, dims, width, reach, pieces=(), kind=jnp.bfloat16):
    factor_of = shard_levels(rng, dims, pieces, -0.22, 0.18) if pieces else 1.0
    result = jax.random.normal(rng, dims, jnp.float32) * width * factor_of
    return jnp.minimum(jnp.maximum(result, -reach), reach).astype(kind)


def bell_draw_with(stream_key, shape, width, most, pieces, heavy, held_as=jnp.bfloat16):
    drawn = width * jax.random.normal(stream_key, shape, jnp.float32)
    if pieces:
        drawn = drawn * shard_levels(stream_key, shape, pieces, -0.22, 0.18)
    return jnp.clip(spiked(drawn, jax.random.fold_in(stream_key, 3), *heavy), -most, most).astype(held_as)


def setup_inputs(seed: int = 0) -> dict:
    keys = jax.random.split(jax.random.key(seed), 4)
    tokens = bell_draw(keys[0], (TOKENS, D_IN), (TOKENS ** -0.5), 0.15625, ((0, 64), (1, 2)))
    weight = bell_draw(keys[1], (D_IN, D_OUT), D_IN ** -0.5, 0.0625, ((0, 2), (1, 64)))
    grad_output = bell_draw_with(keys[2], (TOKENS, D_OUT), 1.0, 6.0, ((0, 4), (1, 32)), (1, 0, 32, 2.75))
    return {"tokens": tokens, "weight": weight, "grad_output": grad_output}


def reference(tokens, weight, grad_output):
    grad_input = jnp.dot(grad_output, weight.T, preferred_element_type=jnp.float32).astype(jnp.bfloat16)
    grad_weight = jnp.dot(tokens.T, grad_output, preferred_element_type=jnp.float32).astype(jnp.bfloat16)
    return grad_input, grad_weight
```

```python
import jax
import jax.numpy as jnp
from jax import lax
from jax.experimental import pallas as pl
from jax.experimental.pallas import tpu as pltpu
from jax.sharding import PartitionSpec as P

MESH = pl.DeviceIdType.MESH
BF16, F32 = jnp.bfloat16, jnp.float32

B = 512
TILE = 256
CODE_ROWS = B + 16
TOP = 320.0
POWER = 15


def encode(tile, ref):
    top = jnp.max(jnp.abs(tile), axis=0, keepdims=True)
    scale = (top * 1.01 + 1e-30).astype(BF16)
    u = tile * (TOP / scale.astype(F32))
    u3 = u * u * u
    u6 = u3 * u3
    ref[0:B, :] = (u6 * u6 * u3).astype(BF16)
    ref[B:CODE_ROWS, :] = jnp.broadcast_to(scale.astype(F32), (16, TILE)).astype(BF16)


def decode(ref):
    code = ref[0:B, :].astype(F32)
    scale = ref[B:CODE_ROWS, :].astype(F32)[0:1] * (1.0 / TOP)
    size = jnp.exp2(jnp.log2(jnp.abs(code)) * (1.0 / POWER))
    return jnp.where(code < 0, -size, size) * scale


def kernel(
    t_hbm, w_hbm, g_hbm, gi_out, gw_out,
    t_loc, tt_loc, tt, w, g, gi_tx, gi_hop, gi_rx, gw_tx, gw_hop, gw_rx, gi_fin, gw_fin,
    local_sem, g_local_sem,
    w_ex_send, t_ex_send, w_ag_send, t_ag_send, w_fw_send, t_fw_send, w_recv, t_recv,
    g_ring_send, g_fw_send, g_mate_send, g_recv, g_mate_recv,
    gi_send, gi_hop_recv, gi_recv, gw_send, gw_hop_recv, gw_recv,
    gi_fin_send, gi_fin_recv, gw_fin_send, gw_fin_recv,
):
    z, col, yl = lax.axis_index("row"), lax.axis_index("col"), lax.axis_index("depth")
    x, q = col // 4, col % 4
    yh, core = q // 2, q % 2
    y = 2 * yh + yl

    def at_x(k):
        return (z, ((x + k) % 4) * 4 + q, yl)

    def at_z(k):
        return ((z + k) % 4, col, yl)

    def at_y(k):
        other = (y + k) % 4
        return (z, x * 4 + (other // 2) * 2 + core, other % 2)

    mate = (z, x * 4 + yh * 2 + (1 - core), yl)

    def partner(k):
        return (z, x * 4 + k, 1 - yl)

    def send(src, dst, send_sem, recv_sem, to):
        copy = pltpu.make_async_remote_copy(
            src_ref=src, dst_ref=dst, send_sem=send_sem, recv_sem=recv_sem, device_id=to, device_id_type=MESH
        )
        copy.start()
        return copy

    def arrived(ref, sem):
        pltpu.make_async_remote_copy(
            src_ref=ref, dst_ref=ref, send_sem=sem, recv_sem=sem, device_id=mate, device_id_type=MESH
        ).wait_recv()

    sent = []

    def lanes(block, k):
        return pl.ds(pl.multiple_of(block * B + k * 128, 128), 128)

    t_copy = pltpu.make_async_copy(t_hbm, t_loc, local_sem)
    t_copy.start()
    g_copies = []
    for e in range(2):
        g_copies.append(
            pltpu.make_async_copy(g_hbm.at[:, pl.ds(e * 128, 128)], g.at[:, lanes(2 * yl + e, q)], g_local_sem.at[e])
        )
        g_copies[-1].start()

    barrier = pltpu.get_barrier_semaphore()
    peers = [at_x(1), at_x(3), at_z(1), at_z(3), mate] + [partner(k) for k in range(4)]
    for peer in peers:
        pl.semaphore_signal(barrier, inc=1, device_id=peer, device_id_type=MESH)
    pl.semaphore_wait(barrier, len(peers))

    for k in range(4):
        sent.append(
            send(w_hbm.at[pl.ds(k * 1024, 1024), :], w.at[:, lanes(z, q)], w_ex_send.at[k], w_recv.at[0, q], partner(k))
        )
    t_copy.wait()
    for k in range(4):
        for part in range(2):
            at = k * 1024 + part * 512
            tt_loc[at : at + 512, :] = t_loc[:, at : at + 512].T
        sent.append(
            send(tt_loc.at[pl.ds(k * 1024, 1024), :], tt.at[:, lanes(x, q)], t_ex_send.at[k], t_recv.at[0, q], partner(k))
        )

    order = (2, 1, 3, 0)

    def g_piece(r, dy, other_core, e):
        owner = (y + dy) % 4
        rows = pl.ds(pl.multiple_of(((x + order[r]) % 4) * B, B), B)
        k = (owner // 2) * 2 + (core if not other_core else 1 - core)
        return g.at[rows, lanes(2 * (owner % 2) + e, k)]

    def g_own(r):
        for e in range(2):
            piece = g_piece(r, 0, False, e)
            sent.append(send(piece, piece, g_ring_send.at[r, 0, e], g_recv.at[r, 0, e], at_y(1)))
            sent.append(send(piece, piece, g_ring_send.at[r, 1, e], g_recv.at[r, 1, e], at_y(3)))

    def g_to_mate(r, dy, slot, e):
        piece = g_piece(r, dy, False, e)
        sent.append(send(piece, piece, g_mate_send.at[r, slot, e], g_mate_recv.at[r, slot, e], mate))

    def g_first(r):
        for e in range(2):
            arrived(g_piece(r, 3, False, e), g_recv.at[r, 0, e])
            if e == 0:
                piece = g_piece(r, 3, False, 0)
                sent.append(send(piece, piece, g_fw_send.at[r, 0], g_recv.at[r, 2, 0], at_y(1)))
            arrived(g_piece(r, 1, False, 1 - e), g_recv.at[r, 1, 1 - e])
            if e == 0:
                piece = g_piece(r, 1, False, 1)
                sent.append(send(piece, piece, g_fw_send.at[r, 1], g_recv.at[r, 2, 1], at_y(3)))
            g_to_mate(r, 3, 1, e)
            g_to_mate(r, 1, 2, 1 - e)

    def g_second(r):
        for e in range(2):
            arrived(g_piece(r, 2, False, e), g_recv.at[r, 2, e])
            g_to_mate(r, 2, 3, e)

    def g_from_mate(r):
        for slot, dy in enumerate((0, 3, 1, 2)):
            for e in range(2):
                arrived(g_piece(r, dy, True, e), g_mate_recv.at[r, slot, e])

    for copy in g_copies:
        copy.wait()
    g_own(0)
    for r in range(4):
        for e in range(2):
            g_to_mate(r, 0, 0, e)
    g_own(1)

    def ring_own(ref, at, me, ag_send, recv, k):
        piece = ref.at[:, lanes(me, k)]
        arrived(piece, recv.at[0, k])
        sent.append(send(piece, piece, ag_send.at[0, k], recv.at[1, k], at(1)))
        sent.append(send(piece, piece, ag_send.at[1, k], recv.at[2, k], at(3)))

    def ring_forward(ref, at, me, fw_send, recv, k):
        if k < 2:
            piece, slot, to = ref.at[:, lanes((me + 3) % 4, k)], 1, at(1)
        else:
            piece, slot, to = ref.at[:, lanes((me + 1) % 4, k)], 2, at(3)
        arrived(piece, recv.at[slot, k])
        sent.append(send(piece, piece, fw_send.at[k], recv.at[3, k], to))

    def ring_rest(ref, me, recv):
        for k in range(4):
            if k >= 2:
                arrived(ref.at[:, lanes((me + 3) % 4, k)], recv.at[1, k])
            else:
                arrived(ref.at[:, lanes((me + 1) % 4, k)], recv.at[2, k])
        for k in range(4):
            arrived(ref.at[:, lanes((me + 2) % 4, k)], recv.at[3, k])

    for k in (0, 2, 1, 3):
        ring_own(w, at_z, z, w_ag_send, w_recv, k)
    for k in (0, 2, 1, 3):
        ring_own(tt, at_x, x, t_ag_send, t_recv, k)
    for k in (0, 2, 1, 3):
        ring_forward(w, at_z, z, w_fw_send, w_recv, k)
    g_first(0)
    g_own(2)
    for k in (0, 2, 1, 3):
        ring_forward(tt, at_x, x, t_fw_send, t_recv, k)
    g_second(0)
    g_first(1)
    g_own(3)
    ring_rest(w, z, w_recv)
    g_from_mate(0)

    def gi_tile(dx, j):
        rows = pl.ds(pl.multiple_of(((x + dx) % 4) * B, B), B)
        return lax.dot_general(
            g[rows, :], w[pl.ds(pl.multiple_of(j * TILE, TILE), TILE), :], (((1,), (1,)), ((), ())),
            preferred_element_type=F32,
        )

    def gw_tile(dz, j):
        rows = pl.ds(pl.multiple_of((j // 2) * B, B), B)
        columns = pl.ds(pl.multiple_of(((z + dz) % 4) * B + (j % 2) * TILE, TILE), TILE)
        return jnp.dot(tt[rows, :], g[:, columns], preferred_element_type=F32)

    class Reduction:
        def __init__(self, tile, at, tx, hop, rx, send_sem, hop_recv, recv):
            self.tile, self.at, self.tx, self.hop, self.rx = tile, at, tx, hop, rx
            self.send_sem, self.hop_recv, self.recv = send_sem, hop_recv, recv

        def far(self):
            @pl.loop(0, 4)
            def _(j):
                encode(self.tile(2, j), self.tx.at[0, j])
                send(self.tx.at[0, j], self.hop.at[j], self.send_sem.at[0, j], self.hop_recv.at[j], self.at(1 + 2 * (j // 2)))

        def near(self):
            @pl.loop(0, 4)
            def _(t):
                side, j = t // 2, (t + 2) % 4
                encode(self.tile(1 + 2 * side, j), self.tx.at[1 + side, j])
                send(
                    self.tx.at[1 + side, j], self.rx.at[side, j], self.send_sem.at[1 + side, j], self.recv.at[side, j],
                    self.at(1 + 2 * side),
                )

        def near_with_far(self):
            @pl.loop(0, 4)
            def _(j):
                side = j // 2
                tile = self.tile(1 + 2 * side, j)
                arrived(self.hop.at[j], self.hop_recv.at[j])
                encode(tile + decode(self.hop.at[j]), self.tx.at[1 + side, j])
                send(
                    self.tx.at[1 + side, j], self.rx.at[side, j], self.send_sem.at[1 + side, j], self.recv.at[side, j],
                    self.at(1 + 2 * side),
                )

        def total(self, j):
            tile = self.tile(0, j)
            for side in range(2):
                arrived(self.rx.at[side, j], self.recv.at[side, j])
                tile = tile + decode(self.rx.at[side, j])
            return tile.astype(BF16)

        def drain(self):
            @pl.loop(0, 4)
            def _(j):
                for k in range(3):
                    ref = self.tx.at[k, j]
                    pltpu.make_async_remote_copy(
                        src_ref=ref, dst_ref=ref, send_sem=self.send_sem.at[k, j], recv_sem=self.send_sem.at[k, j],
                        device_id=mate, device_id_type=MESH,
                    ).wait_send()

    gi = Reduction(gi_tile, at_x, gi_tx, gi_hop, gi_rx, gi_send, gi_hop_recv, gi_recv)
    gw = Reduction(gw_tile, at_z, gw_tx, gw_hop, gw_rx, gw_send, gw_hop_recv, gw_recv)

    gi.far()
    g_second(1)
    g_first(2)
    g_first(3)
    g_from_mate(1)
    g_second(2)
    g_from_mate(2)
    gi.near()
    g_second(3)
    ring_rest(tt, x, t_recv)
    g_from_mate(3)
    gw.far()
    gi.near_with_far()
    gw.near()
    gw.near_with_far()

    def gi_piece(j, k):
        columns = pl.ds(pl.multiple_of(k * 1024 + j * TILE, TILE), TILE)
        return gi_out.at[:, columns]

    @pl.loop(0, 4)
    def _(j):
        gi_fin[j] = gi.total(j)
        for k in range(4):
            send(
                gi_fin.at[j, pl.ds(k * 128, 128), :], gi_piece(j, q), gi_fin_send.at[j, k], gi_fin_recv.at[j, q], partner(k)
            )

    def gw_piece(i, k):
        return gw_out.at[pl.ds(pl.multiple_of(k * 1024 + i * B, B), B), :]

    @pl.loop(0, 4)
    def _(j):
        gw_fin[j] = gw.total(j)
        for e in range(2):
            send(
                gw_fin.at[j, :, pl.ds(e * 128, 128)], gw_piece(j // 2, q), gw_fin_send.at[j, e],
                gw_fin_recv.at[j // 2, q], partner(2 * (j % 2) + e),
            )

    for copy in sent:
        copy.wait_send()
    gi.drain()
    gw.drain()

    @pl.loop(0, 4)
    def _(j):
        for k in range(4):
            pltpu.make_async_remote_copy(
                src_ref=gi_fin.at[j, pl.ds(k * 128, 128), :], dst_ref=gi_piece(j, k), send_sem=gi_fin_send.at[j, k],
                recv_sem=gi_fin_recv.at[j, k], device_id=mate, device_id_type=MESH,
            ).wait()
        for e in range(2):
            pltpu.make_async_remote_copy(
                src_ref=gw_fin.at[j, :, pl.ds(e * 128, 128)], dst_ref=gw_piece(0, 0), send_sem=gw_fin_send.at[j, e],
                recv_sem=gw_fin_send.at[j, e], device_id=mate, device_id_type=MESH,
            ).wait_send()

    for i in range(2):
        for k in range(4):
            arrived(gw_piece(i, k), gw_fin_recv.at[i, k])


def per_device(tokens, weight, grad_output):
    dma = pltpu.SemaphoreType.DMA
    codes = lambda *lead: pltpu.VMEM((*lead, CODE_ROWS, TILE), BF16)
    any_spec = pl.BlockSpec(memory_space=pl.ANY)
    return pl.pallas_call(
        kernel,
        out_shape=(jax.ShapeDtypeStruct((128, 4096), BF16), jax.ShapeDtypeStruct((4096, 128), BF16)),
        in_specs=[any_spec] * 3,
        out_specs=(any_spec, any_spec),
        scratch_shapes=[
            pltpu.VMEM((128, 4096), BF16), pltpu.VMEM((4096, 128), BF16),
            pltpu.VMEM((1024, 2048), BF16), pltpu.VMEM((1024, 2048), BF16), pltpu.VMEM((2048, 2048), BF16),
            codes(3, 4), codes(4), codes(2, 4), codes(3, 4), codes(4), codes(2, 4),
            pltpu.VMEM((4, B, TILE), BF16), pltpu.VMEM((4, B, TILE), BF16),
            dma(()), dma((2,)),
            dma((4,)), dma((4,)), dma((2, 4)), dma((2, 4)), dma((4,)), dma((4,)), dma((4, 4)), dma((4, 4)),
            dma((4, 2, 2)), dma((4, 2)), dma((4, 4, 2)), dma((4, 3, 2)), dma((4, 4, 2)),
            dma((3, 4)), dma((4,)), dma((2, 4)), dma((3, 4)), dma((4,)), dma((2, 4)),
            dma((4, 4)), dma((4, 4)), dma((4, 2)), dma((2, 4)),
        ],
        compiler_params=pltpu.CompilerParams(
            collective_id=0, has_side_effects=True, vmem_limit_bytes=60 * 1024 * 1024
        ),
        name="linear_backward",
    )(tokens, weight, grad_output)


def solution(mesh):
    return jax.shard_map(
        per_device,
        mesh=mesh,
        in_specs=(P(("row", "col"), "depth"), P("depth", ("col", "row")), P("row", ("col", "depth"))),
        out_specs=(P(("row", "col"), "depth"), P("depth", ("col", "row"))),
        check_vma=False,
    )
```

```python
import jax
import jax.numpy as jnp
from jax import lax
from jax.experimental import pallas as pl
from jax.experimental.pallas import tpu as pltpu
from jax.sharding import PartitionSpec as P

MESH = pl.DeviceIdType.MESH
BF16, F32 = jnp.bfloat16, jnp.float32

B = 512
TILE = 256
CODE_ROWS = B + 16
TOP = 320.0
POWER = 15
PARTS = 4
PART = 1024 // PARTS

OWN, RIGHT, FAR, LEFT = 0, 1, 2, 3
TOKEN_SLOT = {FAR: 0, RIGHT: 1, LEFT: 2, OWN: 3}


def weight_lane(member, pair):
    return {FAR: 0, OWN: 256, RIGHT: 1024, LEFT: 1280}[member] + pair * 512


def token_lane(member, pair):
    return TOKEN_SLOT[member] * B + pair * 256


def encode(tile, ref):
    top = jnp.max(jnp.abs(tile), axis=0, keepdims=True)
    scale = (top * 1.01 + 1e-30).astype(BF16)
    u = tile * (TOP / scale.astype(F32))
    u3 = u * u * u
    u6 = u3 * u3
    ref[0:B, :] = (u6 * u6 * u3).astype(BF16)
    ref[B:CODE_ROWS, :] = jnp.broadcast_to(scale.astype(F32), (16, TILE)).astype(BF16)


def decode(ref):
    code = ref[0:B, :].astype(F32)
    scale = ref[B:CODE_ROWS, :].astype(F32)[0:1] * (1.0 / TOP)
    size = jnp.exp2(jnp.log2(jnp.abs(code)) * (1.0 / POWER))
    return jnp.where(code < 0, -size, size) * scale


class Reduction:
    def __init__(self, send, arrived, at, far_tx, hop, tx, rx, far_send, hop_recv, send_sem, recv):
        self.send, self.arrived, self.at, self.far_tx, self.hop, self.tx, self.rx = send, arrived, at, far_tx, hop, tx, rx
        self.far_send, self.hop_recv, self.send_sem, self.recv = far_send, hop_recv, send_sem, recv

    def half(self, ref, j, side):
        return ref.at[j, :, pl.ds(side * 128, 128)]

    def far(self, tile, j):
        encode(tile, self.far_tx.at[j])

    def far_start(self, j):
        for side in range(2):
            self.send(
                self.half(self.far_tx, j, side), self.half(self.hop, j, side), self.far_send,
                self.hop_recv.at[side, j], self.at(1 + 2 * side),
            )

    def near_wait(self, j):
        for side in range(2):
            self.arrived(self.half(self.hop, j, side), self.hop_recv.at[side, j])

    def near(self, tile, j, side):
        parts = [tile[:, 0:128], tile[:, 128:256]]
        parts[side] = parts[side] + decode(self.half(self.hop, j, side))
        encode(jnp.concatenate(parts, axis=1), self.tx.at[side, j])

    def near_start(self, j):
        for side in range(2):
            self.send(
                self.tx.at[side, j], self.rx.at[side, j], self.send_sem, self.recv.at[side, j],
                self.at(1 + 2 * side),
            )

    def total_wait(self, j):
        for side in range(2):
            self.arrived(self.rx.at[side, j], self.recv.at[side, j])

    def total(self, tile, j):
        return (tile + decode(self.rx.at[0, j]) + decode(self.rx.at[1, j])).astype(BF16)

    def drain(self, sent_from):
        sent_from(self.far_tx, self.far_send)
        sent_from(self.tx, self.send_sem)


def kernel(
    t_hbm, w_hbm, g_hbm, gi_all, gw_all,
    t_loc, tt_loc, tt, w, g, gi_far_tx, gi_hop, gi_tx, gi_rx, gw_far_tx, gw_hop, gw_tx, gw_rx, gi_fin, gw_fin, gw_own, gi_own, gi_part, gw_part,
    local_sem, g_local_sem,
    w_ex_send, t_ex_send, w_ex_recv, t_ex_recv, w_ag_send, t_ag_send, w_fw_send, t_fw_send, w_recv, t_recv, w_rest, t_rest,
    g_ring_send, g_fw_send, g_mate_send, g_recv, g_mate_recv,
    gi_far_send, gi_hop_recv, gi_send, gi_recv, gw_far_send, gw_hop_recv, gw_send, gw_recv,
    gi_fin_send, gi_fin_recv, gw_fin_send, gw_fin_recv,
):
    z, col, yl = lax.axis_index("row"), lax.axis_index("col"), lax.axis_index("depth")
    x, q = col // 4, col % 4
    yh, core = q // 2, q % 2
    y = 2 * yh + yl

    def at_x(k):
        return (z, ((x + k) % 4) * 4 + q, yl)

    def at_z(k):
        return ((z + k) % 4, col, yl)

    def at_y(k):
        other = (y + k) % 4
        return (z, x * 4 + (other // 2) * 2 + core, other % 2)

    mate = (z, x * 4 + yh * 2 + (1 - core), yl)

    def partner(k):
        return (z, x * 4 + k, 1 - yl)

    def send(src, dst, send_sem, recv_sem, to):
        copy = pltpu.make_async_remote_copy(
            src_ref=src, dst_ref=dst, send_sem=send_sem, recv_sem=recv_sem, device_id=to, device_id_type=MESH
        )
        copy.start()

    def arrived(ref, sem):
        pltpu.make_async_remote_copy(
            src_ref=ref, dst_ref=ref, send_sem=sem, recv_sem=sem, device_id=mate, device_id_type=MESH
        ).wait_recv()

    def sent_from(ref, sem):
        pltpu.make_async_remote_copy(
            src_ref=ref, dst_ref=ref, send_sem=sem, recv_sem=sem, device_id=mate, device_id_type=MESH
        ).wait_send()

    steps = ((FAR, 0), (FAR, 1), (RIGHT, 0), (LEFT, 0), (OWN, 0), (RIGHT, 1), (LEFT, 1), (OWN, 1))

    def g_lane(owner, owner_core, late):
        member = (2 * (owner % 2) + (z + late) % 2 - z + 4) % 4
        second = (1 - member // 2) if late == 0 else member // 2
        return pl.multiple_of(late * 1024 + (owner // 2) * 512 + second * 256 + owner_core * 128, 128)

    def g_piece(s, dy, other_core=False, half=None):
        member, late = steps[s]
        start, size = TOKEN_SLOT[member] * B, B
        if half is not None:
            start, size = start + half * (B // 2), B // 2
        lane = g_lane((y + dy) % 4, (1 - core) if other_core else core, late)
        return g.at[pl.ds(start, size), pl.ds(lane, 128)]

    t_copy = pltpu.make_async_copy(t_hbm, t_loc, local_sem)
    t_copy.start()
    for s, (member, late) in enumerate(steps):
        rows = pl.ds(pl.multiple_of(((x + member) % 4) * B, B), B)
        columns = pl.ds(pl.multiple_of(((z + late) % 2) * 128, 128), 128)
        pltpu.make_async_copy(g_hbm.at[rows, columns], g_piece(s, 0), g_local_sem).start()

    barrier = pltpu.get_barrier_semaphore()
    peers = [at_x(1), at_x(3), at_z(1), at_z(3), mate] + [partner(k) for k in range(4)]
    for peer in peers:
        pl.semaphore_signal(barrier, inc=1, device_id=peer, device_id_type=MESH)
    with jax.named_scope("s00_barrier"):
        pl.semaphore_wait(barrier, len(peers))

    def part_rows(part):
        return pl.ds(part * PART, PART)

    def exchange(src, ref, lane, ex_send, ex_recv, part):
        for k in range(4):
            piece = src.at[pl.ds(k * 1024 + part * PART, PART), :]
            send(piece, ref.at[part_rows(part), pl.ds(lane, 128)], ex_send, ex_recv.at[part, q // 2], partner(k))

    w_own_lane = pl.multiple_of((q // 2) * 512 + 256 + (q % 2) * 128, 128)
    t_own_lane = pl.multiple_of(TOKEN_SLOT[OWN] * B + q * 128, 128)
    exchange(w_hbm, w, w_own_lane, w_ex_send, w_ex_recv, 0)
    t_copy.wait()
    for k in range(8):
        tt_loc[k * 512 : k * 512 + 512, :] = t_loc[:, k * 512 : k * 512 + 512].T
    exchange(tt_loc, tt, t_own_lane, t_ex_send, t_ex_recv, 0)
    for part in range(1, PARTS):
        exchange(w_hbm, w, w_own_lane, w_ex_send, w_ex_recv, part)
        exchange(tt_loc, tt, t_own_lane, t_ex_send, t_ex_recv, part)

    def g_own(s):
        piece = g_piece(s, 0)
        send(piece, piece, g_ring_send, g_recv.at[s, 0], at_y(1))
        send(piece, piece, g_ring_send, g_recv.at[s, 1], at_y(3))

    def g_to_mate(s, dy):
        piece = g_piece(s, dy)
        send(piece, piece, g_mate_send, g_mate_recv.at[s], mate)

    def g_first(s):
        for side, dy in ((0, 3), (1, 1)):
            arrived(g_piece(s, dy), g_recv.at[s, side])
            piece = g_piece(s, dy, half=side)
            send(piece, piece, g_fw_send, g_recv.at[s, 2], at_y(1 + 2 * side))
            g_to_mate(s, dy)

    def g_second(s):
        arrived(g_piece(s, 2), g_recv.at[s, 2])
        g_to_mate(s, 2)

    def g_from_mate(s):
        arrived(g.at[0:B, 0:512], g_mate_recv.at[s])

    pltpu.make_async_copy(tt_loc, tt_loc, g_local_sem).wait()
    g_own(0)
    for s in range(8):
        g_to_mate(s, 0)
    g_own(1)

    class Ring:
        def __init__(self, ref, lane, at, ex_recv, ag_send, fw_send, recv, rest_recv):
            self.ref, self.lane, self.at = ref, lane, at
            self.ex_recv, self.ag_send, self.fw_send, self.recv, self.rest_recv = ex_recv, ag_send, fw_send, recv, rest_recv

        def piece(self, member, part, pair):
            return self.ref.at[part_rows(part), pl.ds(self.lane(member, pair), 256)]

        def own(self, part):
            for pair in range(2):
                piece = self.piece(OWN, part, pair)
                arrived(piece, self.ex_recv.at[part, pair])
                for side, member in ((0, LEFT), (1, RIGHT)):
                    kept = (part < PARTS // 2) == (side == 1)
                    sem = self.rest_recv.at[0] if kept else self.recv.at[part, pair]
                    send(piece, self.piece(member, part, pair), self.ag_send, sem, self.at(1 + 2 * side))

        def forward(self, part):
            side = 0 if part < PARTS // 2 else 1
            for pair in range(2):
                piece = self.piece((LEFT, RIGHT)[side], part, pair)
                arrived(piece, self.recv.at[part, pair])
                send(piece, self.piece(FAR, part, pair), self.fw_send, self.rest_recv.at[1], self.at(1 + 2 * side))

        def rest(self):
            for k in range(2):
                arrived(self.ref.at[:, 0:512], self.rest_recv.at[k])

        def drain(self):
            sent_from(self.ref.at[:, 0:1024], self.ag_send)
            sent_from(self.ref.at[:, 0:512], self.fw_send)

    w_ring = Ring(w, weight_lane, at_z, w_ex_recv, w_ag_send, w_fw_send, w_recv, w_rest)
    t_ring = Ring(tt, token_lane, at_x, t_ex_recv, t_ag_send, t_fw_send, t_recv, t_rest)

    with jax.named_scope("s02_own01"):
        w_ring.own(0)
        t_ring.own(0)
        w_ring.own(1)
    with jax.named_scope("s03_own12"):
        t_ring.own(1)
        w_ring.forward(0)
        w_ring.own(2)
        t_ring.forward(0)
        t_ring.own(2)
    with jax.named_scope("s04_own3"):
        w_ring.forward(1)
        w_ring.own(3)
        t_ring.forward(1)
        t_ring.own(3)
    with jax.named_scope("s05_wfw2"):
        w_ring.forward(2)
    with jax.named_scope("s08_g0"):
        g_first(0)
        g_own(2)
    with jax.named_scope("s09_tfw2wfw3"):
        t_ring.forward(2)
        w_ring.forward(3)
    with jax.named_scope("s10_g1"):
        g_first(1)
        g_own(3)
        g_second(0)
    with jax.named_scope("s11_tfw3"):
        t_ring.forward(3)
    with jax.named_scope("s12_g2"):
        g_first(2)
        g_own(4)
        g_second(1)
    with jax.named_scope("s13_g3"):
        g_first(3)
        g_own(5)
        g_second(2)
    with jax.named_scope("s14_wrest"):
        w_ring.rest()
    with jax.named_scope("s15_gm01"):
        g_from_mate(0)
        g_from_mate(1)

    by_rows = (((1,), (1,)), ((), ()))

    HALF = 1024

    def gi_dot(slot, slots, j, tiles, first=0, terms=2 * HALF):
        return lax.dot_general(
            g[slot * B : (slot + slots) * B, first : first + terms],
            w[pl.ds(pl.multiple_of(j * TILE, TILE), tiles * TILE), first : first + terms],
            by_rows, preferred_element_type=F32,
        )

    def gw_dot(lane, j, first=0, terms=2 * HALF):
        rows = pl.ds(pl.multiple_of((j // 2) * B, B), B)
        columns = pl.ds(pl.multiple_of(lane + (j % 2) * 512, 512), 512)
        return jnp.dot(tt[rows, first : first + terms], g[first : first + terms, columns], preferred_element_type=F32)

    gi = Reduction(send, arrived, at_x, gi_far_tx, gi_hop, gi_tx, gi_rx, gi_far_send, gi_hop_recv, gi_send, gi_recv)
    gw = Reduction(send, arrived, at_z, gw_far_tx, gw_hop, gw_tx, gw_rx, gw_far_send, gw_hop_recv, gw_send, gw_recv)

    def gi_far_pair(j):
        both = gi_dot(0, 1, j, 2)
        for k in range(2):
            gi.far(both[:, k * TILE : (k + 1) * TILE], j + k)
        for k in range(2):
            gi.far_start(j + k)

    def gw_columns_dot(lane, half):
        columns = pl.ds(pl.multiple_of(lane + half * 512, 256), TILE)
        return jnp.dot(tt[...], g[:, columns], preferred_element_type=F32)

    def gw_far_pair(half):
        columns = pl.ds(pl.multiple_of(half * 512, 256), TILE)
        for k in range(2):
            tile = jnp.dot(tt[k * B : (k + 1) * B, :], g[:, columns], preferred_element_type=F32)
            gw.far(tile, 2 * k + half)
        for k in range(2):
            gw.far_start(2 * k + half)

    def gw_own_all():
        @pl.loop(0, 2)
        def _(half):
            both = gw_columns_dot(TILE, half)
            for k in range(2):
                gw_own[2 * k + half] = both[k * B : (k + 1) * B]

    def gi_near_part(h):
        both = gi_dot(1, 2, 2 * h, 2, 0, HALF)
        for side in range(2):
            for k in range(2):
                gi_part[side, 2 * h + k] = both[side * B : (side + 1) * B, k * TILE : (k + 1) * TILE]

    def gi_own_part():
        @pl.loop(0, 2)
        def _(h):
            both = gi_dot(3, 1, 2 * h, 2, 0, HALF)
            for k in range(2):
                gi_own[2 * h + k] = both[:, k * TILE : (k + 1) * TILE]

    def gw_near_part(j):
        gw_part[j] = gw_dot(1024, j, 0, HALF)

    def gi_near(j):
        gi.near_wait(j)
        for side in range(2):
            tile = gi_part[side, j] + gi_dot(1 + side, 1, j, 1, HALF, HALF)
            gi.near(tile, j, side)
        gi.near_start(j)

    def gw_near(j):
        gw.near_wait(j)
        both = gw_part[j] + gw_dot(1024, j, HALF, HALF)
        for side in range(2):
            gw.near(both[:, side * TILE : (side + 1) * TILE], j, side)
        gw.near_start(j)

    def gi_piece(j, k):
        return gi_all.at[:, pl.ds(pl.multiple_of(k * 1024 + j * TILE, TILE), TILE)]

    def gw_piece(i, k):
        return gw_all.at[pl.ds(pl.multiple_of(k * 1024 + i * B, B), B), :]

    def gi_final(j):
        tile = gi_own[j] + gi_dot(3, 1, j, 1, HALF, HALF)
        gi.total_wait(j)
        gi_fin[j] = gi.total(tile, j)
        for k in range(4):
            send(
                gi_fin.at[j, pl.ds(k * 128, 128), :], gi_piece(j, q), gi_fin_send, gi_fin_recv,
                partner(k),
            )

    def gw_final(j):
        gw.total_wait(j)
        gw_fin[j] = gw.total(gw_own[j], j)
        for e in range(2):
            send(
                gw_fin.at[j, :, pl.ds(e * 128, 128)], gw_piece(j // 2, q), gw_fin_send,
                gw_fin_recv, partner(2 * (j % 2) + e),
            )

    def steps_of(count, work, after, name):
        @pl.loop(0, count)
        def _(h):
            with jax.named_scope(name):
                work(h)
            for at, service in after.items():

                @pl.when(h == at)
                def _():
                    with jax.named_scope(name + "_g"):
                        service()

    def forward_4():
        g_first(4)
        g_own(6)

    def forward_5():
        g_first(5)
        g_own(7)

    steps_of(2, lambda h: gi_far_pair(2 * h), {0: forward_4, 1: lambda: g_second(3)}, "s16_gifar")
    with jax.named_scope("s17_gm23"):
        g_from_mate(2)
        g_from_mate(3)
    steps_of(2, gi_near_part, {0: forward_5, 1: lambda: g_second(4)}, "s18_gipart")
    with jax.named_scope("s19_trest"):
        t_ring.rest()
        g_from_mate(4)
    steps_of(2, gw_far_pair, {0: lambda: g_first(6), 1: lambda: g_second(5)}, "s20_gwfar")
    with jax.named_scope("s21_gm5"):
        g_from_mate(5)
    steps_of(4, gw_near_part, {1: lambda: g_first(7), 3: lambda: g_second(6)}, "s22_gwpart")
    with jax.named_scope("s23_giown"):
        gi_own_part()
    with jax.named_scope("s24_g7"):
        g_second(7)
        g_from_mate(6)

    @pl.loop(0, 5)
    def _(j):
        @pl.when(j < 4)
        def _():
            with jax.named_scope("s31_ginear"):
                gi_near(j)

        @pl.when(j == 0)
        def _():
            with jax.named_scope("s30_gm7"):
                g_from_mate(7)

        @pl.when(j < 4)
        def _():
            with jax.named_scope("s33_gwnear"):
                gw_near(j)

        @pl.when(j == 1)
        def _():
            with jax.named_scope("s34_gwown"):
                gw_own_all()

        @pl.when(j > 0)
        def _():
            with jax.named_scope("s35_gifinal"):
                gi_final(j - 1)
            with jax.named_scope("s36_gwfinal"):
                gw_final(j - 1)

    with jax.named_scope("s50_drain"):
        for src, sem in ((w_hbm, w_ex_send), (tt_loc, t_ex_send), (gi_fin, gi_fin_send), (gw_fin, gw_fin_send)):
            sent_from(src, sem)
        sent_from(g.at[0:B, :], g_ring_send)
        sent_from(g.at[0:B, 0:1024], g_fw_send)
        sent_from(g.at[:, 0:1024], g_mate_send)
        w_ring.drain()
        t_ring.drain()
        gi.drain(sent_from)
        gw.drain(sent_from)
    with jax.named_scope("s52_giout"):
        arrived(gi_all, gi_fin_recv)
    with jax.named_scope("s53_gwout"):
        arrived(gw_all, gw_fin_recv)


def per_device(tokens, weight, grad_output):
    dma = pltpu.SemaphoreType.DMA
    codes = lambda *lead: pltpu.VMEM((*lead, CODE_ROWS, TILE), BF16)
    any_spec = pl.BlockSpec(memory_space=pl.ANY)
    return pl.pallas_call(
        kernel,
        out_shape=(pltpu.VMEM((128, 4096), BF16), pltpu.VMEM((4096, 128), BF16)),
        in_specs=[any_spec] * 3,
        out_specs=(any_spec, any_spec),
        scratch_shapes=[
            pltpu.VMEM((128, 4096), BF16), pltpu.VMEM((4096, 128), BF16),
            pltpu.VMEM((1024, 2048), BF16), pltpu.VMEM((1024, 2048), BF16), pltpu.VMEM((2048, 2048), BF16),
            codes(4), codes(4), codes(2, 4), codes(2, 4), codes(4), codes(4), codes(2, 4), codes(2, 4),
            pltpu.VMEM((4, B, TILE), BF16), pltpu.VMEM((4, B, TILE), BF16), pltpu.VMEM((4, B, TILE), F32),
            pltpu.VMEM((4, B, TILE), F32), pltpu.VMEM((2, 4, B, TILE), F32), pltpu.VMEM((4, B, 2 * TILE), F32),
            dma(()), dma(()),
            dma(()), dma(()), dma((PARTS, 2)), dma((PARTS, 2)),
            dma(()), dma(()), dma(()), dma(()), dma((PARTS, 2)), dma((PARTS, 2)), dma((2,)), dma((2,)),
            dma(()), dma(()), dma(()), dma((8, 3)), dma((8,)),
            dma(()), dma((2, 4)), dma(()), dma((2, 4)), dma(()), dma((2, 4)), dma(()), dma((2, 4)),
            dma(()), dma(()), dma(()), dma(()),
        ],
        compiler_params=pltpu.CompilerParams(
            collective_id=0, has_side_effects=True, vmem_limit_bytes=58 * 1024 * 1024
        ),
        name="linear_backward",
    )(tokens, weight, grad_output)


def solution(mesh):
    return jax.shard_map(
        per_device,
        mesh=mesh,
        in_specs=(P(("row", "col"), "depth"), P("depth", ("col", "row")), P("row", ("col", "depth"))),
        out_specs=(P(("row", "col"), "depth"), P("depth", ("col", "row"))),
        check_vma=False,
    )
```

```python
import jax
import jax.numpy as jnp
from jax import lax
from jax.experimental import pallas as pl
from jax.experimental.pallas import tpu as pltpu
from jax.sharding import PartitionSpec as P

MESH = pl.DeviceIdType.MESH
BF16, F32 = jnp.bfloat16, jnp.float32

B = 512
TILE = 256
CODE_ROWS = B + 8
TOP = 320.0
POWER = 15
PARTS = 4
PART = 1024 // PARTS

OWN, RIGHT, FAR, LEFT = 0, 1, 2, 3
TOKEN_SLOT = {FAR: 0, RIGHT: 1, LEFT: 2, OWN: 3}


def weight_lane(member, pair):
    return {FAR: 0, OWN: 256, RIGHT: 1024, LEFT: 1280}[member] + pair * 512


def token_lane(member, pair):
    return TOKEN_SLOT[member] * B + pair * 256


def encode(tile, ref):
    top = jnp.max(jnp.abs(tile), axis=0, keepdims=True)
    scale = (top * 1.01 + 1e-30).astype(BF16)
    u = tile * (TOP / scale.astype(F32))
    u3 = u * u * u
    u6 = u3 * u3
    ref[0:B, :] = (u6 * u6 * u3).astype(BF16)
    ref[B:CODE_ROWS, :] = jnp.broadcast_to(scale.astype(F32), (8, tile.shape[1])).astype(BF16)


def decode(ref):
    code = ref[0:B, :].astype(F32)
    scale = ref[B:CODE_ROWS, :].astype(F32)[0:1] * (1.0 / TOP)
    size = jnp.exp2(jnp.log2(jnp.abs(code)) * (1.0 / POWER))
    return jnp.where(code < 0, -size, size) * scale


class Reduction:
    def __init__(self, send, arrived, at, far_tx, hop, tx, rx, far_send, hop_recv, send_sem, recv):
        self.send, self.arrived, self.at, self.far_tx, self.hop, self.tx, self.rx = send, arrived, at, far_tx, hop, tx, rx
        self.far_send, self.hop_recv, self.send_sem, self.recv = far_send, hop_recv, send_sem, recv

    def half(self, ref, j, side):
        return ref.at[j, :, pl.ds(side * 128, 128)]

    def far(self, tile, j):
        encode(tile, self.far_tx.at[j])

    def far_start(self, j):
        for side in range(2):
            self.send(
                self.half(self.far_tx, j, side), self.half(self.hop, j, side), self.far_send,
                self.hop_recv.at[side, j], self.at(1 + 2 * side),
            )

    def near_wait(self, j, side):
        self.arrived(self.half(self.hop, j, side), self.hop_recv.at[side, j])

    def near(self, tile, j, side):
        parts = [tile[:, 0:128], tile[:, 128:256]]
        parts[side] = parts[side] + decode(self.half(self.hop, j, side))
        encode(jnp.concatenate(parts, axis=1), self.tx.at[side, j])

    def near_start(self, j, side):
        for e in range(2):
            self.send(
                self.half(self.tx.at[side], j, e), self.half(self.rx.at[side], j, e), self.send_sem,
                self.recv.at[side, j, e], self.at(1 + 2 * side),
            )

    def total(self, own, j, e):
        for side in range(2):
            self.arrived(self.half(self.rx.at[side], j, e), self.recv.at[side, j, e])
        return (own + decode(self.half(self.rx.at[0], j, e)) + decode(self.half(self.rx.at[1], j, e))).astype(BF16)

    def drain(self, sent_from):
        sent_from(self.far_tx, self.far_send)
        sent_from(self.tx, self.send_sem)


def kernel(
    t_hbm, w_hbm, g_hbm, gi_all, gw_all,
    t_loc, w_loc, tt_loc, tt, w, g, gi_far_tx, gi_hop, gi_tx, gi_rx, gw_far_tx, gw_hop, gw_tx, gw_rx, gi_fin, gw_fin, gw_fin_own, gi_own, gi_part, gw_part,
    local_sem, w_local_sem, g_local_sem,
    w_ex_send, t_ex_send, w_ex_recv, t_ex_recv, w_ag_send, t_ag_send, w_fw_send, t_fw_send, w_recv, t_recv, w_rest, t_rest,
    g_ring_send, g_fw_send, g_mate_send, g_recv, g_mate_recv,
    gi_far_send, gi_hop_recv, gi_send, gi_recv, gw_far_send, gw_hop_recv, gw_send, gw_recv,
    gi_fin_send, gi_fin_recv, gw_fin_send, gw_fin_recv,
):
    z, col, yl = lax.axis_index("row"), lax.axis_index("col"), lax.axis_index("depth")
    x, q = col // 4, col % 4
    yh, core = q // 2, q % 2
    y = 2 * yh + yl

    def at_x(k):
        return (z, ((x + k) % 4) * 4 + q, yl)

    def at_z(k):
        return ((z + k) % 4, col, yl)

    def at_y(k):
        other = (y + k) % 4
        return (z, x * 4 + (other // 2) * 2 + core, other % 2)

    mate = (z, x * 4 + yh * 2 + (1 - core), yl)

    def partner(k):
        return (z, x * 4 + k, 1 - yl)

    def send(src, dst, send_sem, recv_sem, to):
        copy = pltpu.make_async_remote_copy(
            src_ref=src, dst_ref=dst, send_sem=send_sem, recv_sem=recv_sem, device_id=to, device_id_type=MESH
        )
        copy.start()

    def arrived(ref, sem):
        pltpu.make_async_remote_copy(
            src_ref=ref, dst_ref=ref, send_sem=sem, recv_sem=sem, device_id=mate, device_id_type=MESH
        ).wait_recv()

    def sent_from(ref, sem):
        pltpu.make_async_remote_copy(
            src_ref=ref, dst_ref=ref, send_sem=sem, recv_sem=sem, device_id=mate, device_id_type=MESH
        ).wait_send()

    steps = ((FAR, 0), (FAR, 1), (RIGHT, 0), (LEFT, 0), (OWN, 0), (RIGHT, 1), (LEFT, 1), (OWN, 1))

    def g_lane(owner, owner_core, late):
        member = (2 * (owner % 2) + (z + late) % 2 - z + 4) % 4
        second = (1 - member // 2) if late == 0 else member // 2
        return pl.multiple_of(late * 1024 + (owner // 2) * 512 + second * 256 + owner_core * 128, 128)

    def g_piece(s, dy, other_core=False, half=None):
        member, late = steps[s]
        start, size = TOKEN_SLOT[member] * B, B
        if half is not None:
            start, size = start + half * (B // 2), B // 2
        lane = g_lane((y + dy) % 4, (1 - core) if other_core else core, late)
        return g.at[pl.ds(start, size), pl.ds(lane, 128)]

    w_copy = pltpu.make_async_copy(w_hbm, w_loc, w_local_sem)
    w_copy.start()
    t_copy = pltpu.make_async_copy(t_hbm, t_loc, local_sem)
    t_copy.start()
    for s, (member, late) in enumerate(steps):
        rows = pl.ds(pl.multiple_of(((x + member) % 4) * B, B), B)
        columns = pl.ds(pl.multiple_of(((z + late) % 2) * 128, 128), 128)
        pltpu.make_async_copy(g_hbm.at[rows, columns], g_piece(s, 0), g_local_sem).start()

    barrier = pltpu.get_barrier_semaphore()
    peers = [at_x(1), at_x(3), at_z(1), at_z(3), mate] + [partner(k) for k in range(4)]
    for peer in peers:
        pl.semaphore_signal(barrier, inc=1, device_id=peer, device_id_type=MESH)
    with jax.named_scope("s00_barrier"):
        pl.semaphore_wait(barrier, len(peers))

    def part_rows(part):
        return pl.ds(part * PART, PART)

    def exchange(src, ref, lane, ex_send, ex_recv, part):
        for k in range(4):
            piece = src.at[pl.ds(k * 1024 + part * PART, PART), :]
            send(piece, ref.at[part_rows(part), pl.ds(lane, 128)], ex_send, ex_recv.at[part, q // 2], partner(k))

    w_own_lane = pl.multiple_of((q // 2) * 512 + 256 + (q % 2) * 128, 128)
    t_own_lane = pl.multiple_of(TOKEN_SLOT[OWN] * B + q * 128, 128)
    w_copy.wait()
    exchange(w_loc, w, w_own_lane, w_ex_send, w_ex_recv, 0)
    t_copy.wait()
    for k in range(8):
        tt_loc[k * 512 : k * 512 + 512, :] = t_loc[:, k * 512 : k * 512 + 512].T
    exchange(tt_loc, tt, t_own_lane, t_ex_send, t_ex_recv, 0)
    for part in range(1, PARTS):
        exchange(w_loc, w, w_own_lane, w_ex_send, w_ex_recv, part)
        exchange(tt_loc, tt, t_own_lane, t_ex_send, t_ex_recv, part)

    def g_own(s):
        piece = g_piece(s, 0)
        send(piece, piece, g_ring_send, g_recv.at[s, 0], at_y(1))
        send(piece, piece, g_ring_send, g_recv.at[s, 1], at_y(3))

    def g_to_mate(s, dy):
        piece = g_piece(s, dy)
        send(piece, piece, g_mate_send, g_mate_recv.at[s], mate)

    def g_forward(s):
        for side, dy in ((0, 3), (1, 1)):
            arrived(g_piece(s, dy), g_recv.at[s, side])
            piece = g_piece(s, dy, half=side)
            send(piece, piece, g_fw_send, g_recv.at[s, 2], at_y(1 + 2 * side))

    def g_first_to_mate(s):
        for dy in (3, 1):
            g_to_mate(s, dy)

    def g_first(s):
        g_forward(s)
        g_first_to_mate(s)

    def g_second(s):
        arrived(g_piece(s, 2), g_recv.at[s, 2])
        g_to_mate(s, 2)

    def g_from_mate(s):
        arrived(g.at[0:B, 0:512], g_mate_recv.at[s])

    pltpu.make_async_copy(tt_loc, tt_loc, g_local_sem).wait()
    g_own(0)
    for s in range(8):
        g_to_mate(s, 0)
    g_own(1)

    class Ring:
        def __init__(self, ref, lane, at, ex_recv, ag_send, fw_send, recv, rest_recv):
            self.ref, self.lane, self.at = ref, lane, at
            self.ex_recv, self.ag_send, self.fw_send, self.recv, self.rest_recv = ex_recv, ag_send, fw_send, recv, rest_recv

        def piece(self, member, part, pair):
            return self.ref.at[part_rows(part), pl.ds(self.lane(member, pair), 256)]

        def own(self, part):
            for pair in range(2):
                piece = self.piece(OWN, part, pair)
                arrived(piece, self.ex_recv.at[part, pair])
                for side, member in ((0, LEFT), (1, RIGHT)):
                    kept = (part < PARTS // 2) == (side == 1)
                    sem = self.rest_recv.at[0] if kept else self.recv.at[part, pair]
                    send(piece, self.piece(member, part, pair), self.ag_send, sem, self.at(1 + 2 * side))

        def forward(self, part):
            side = 0 if part < PARTS // 2 else 1
            for pair in range(2):
                piece = self.piece((LEFT, RIGHT)[side], part, pair)
                arrived(piece, self.recv.at[part, pair])
                send(piece, self.piece(FAR, part, pair), self.fw_send, self.rest_recv.at[1], self.at(1 + 2 * side))

        def rest(self):
            for k in range(2):
                arrived(self.ref.at[:, 0:512], self.rest_recv.at[k])

        def drain(self):
            sent_from(self.ref.at[:, 0:1024], self.ag_send)
            sent_from(self.ref.at[:, 0:512], self.fw_send)

    w_ring = Ring(w, weight_lane, at_z, w_ex_recv, w_ag_send, w_fw_send, w_recv, w_rest)
    t_ring = Ring(tt, token_lane, at_x, t_ex_recv, t_ag_send, t_fw_send, t_recv, t_rest)

    with jax.named_scope("s02_own01"):
        w_ring.own(0)
        t_ring.own(0)
        w_ring.own(1)
    with jax.named_scope("s03_own12"):
        t_ring.own(1)
        w_ring.forward(0)
        w_ring.own(2)
        t_ring.forward(0)
        t_ring.own(2)
    with jax.named_scope("s04_own3"):
        w_ring.forward(1)
        w_ring.own(3)
        t_ring.forward(1)
        t_ring.own(3)
    with jax.named_scope("s05_wfw2"):
        w_ring.forward(2)
    with jax.named_scope("s08_g0"):
        g_first(0)
        g_own(2)
    with jax.named_scope("s09_tfw2wfw3"):
        t_ring.forward(2)
        w_ring.forward(3)
    with jax.named_scope("s10_g1"):
        g_first(1)
        g_own(3)
        g_second(0)
    with jax.named_scope("s11_tfw3"):
        t_ring.forward(3)
    with jax.named_scope("s12_g2"):
        g_first(2)
        g_own(4)
        g_second(1)
    with jax.named_scope("s13_g3"):
        g_first(3)
        g_own(5)
        g_second(2)
    with jax.named_scope("s14_wrest"):
        w_ring.rest()
    with jax.named_scope("s15_gm01"):
        g_from_mate(0)
        g_from_mate(1)

    by_rows = (((1,), (1,)), ((), ()))

    HALF = 1024

    def gi_dot(slot, slots, j, tiles, first=0, terms=2 * HALF):
        return lax.dot_general(
            g[slot * B : (slot + slots) * B, first : first + terms],
            w[pl.ds(pl.multiple_of(j * TILE, TILE), tiles * TILE), first : first + terms],
            by_rows, preferred_element_type=F32,
        )

    def gw_dot(lane, j, first=0, terms=2 * HALF):
        rows = pl.ds(pl.multiple_of((j // 2) * B, B), B)
        columns = pl.ds(pl.multiple_of(lane + (j % 2) * 512, 512), 512)
        return jnp.dot(tt[rows, first : first + terms], g[first : first + terms, columns], preferred_element_type=F32)

    gi = Reduction(send, arrived, at_x, gi_far_tx, gi_hop, gi_tx, gi_rx, gi_far_send, gi_hop_recv, gi_send, gi_recv)
    gw = Reduction(send, arrived, at_z, gw_far_tx, gw_hop, gw_tx, gw_rx, gw_far_send, gw_hop_recv, gw_send, gw_recv)

    def gi_far_pair(j):
        both = gi_dot(0, 1, j, 2)
        for k in range(2):
            gi.far(both[:, k * TILE : (k + 1) * TILE], j + k)
        for k in range(2):
            gi.far_start(j + k)

    def gw_far(t):
        j = 2 * (t % 2) + t // 2
        rows = pl.ds(pl.multiple_of((t % 2) * B, B), B)
        columns = pl.ds(pl.multiple_of((t // 2) * 512, 512), TILE)
        gw.far(jnp.dot(tt[rows, :], g[:, columns], preferred_element_type=F32), j)
        gw.far_start(j)

    def gw_own(j):
        rows = pl.ds(pl.multiple_of((j // 2) * B, B), B)
        columns = pl.ds(pl.multiple_of((j % 2) * 512 + TILE, TILE), TILE)
        return jnp.dot(tt[rows, :], g[:, columns], preferred_element_type=F32)

    def gi_near_part(h):
        both = gi_dot(1, 2, 2 * h, 2, 0, HALF)
        for side in range(2):
            for k in range(2):
                gi_part[side, 2 * h + k] = both[side * B : (side + 1) * B, k * TILE : (k + 1) * TILE]

    def gi_own_all():
        @pl.loop(0, 2)
        def _(h):
            both = gi_dot(3, 1, 2 * h, 2)
            for k in range(2):
                gi_own[2 * h + k] = both[:, k * TILE : (k + 1) * TILE]

    def gw_near_part(j):
        gw_part[j] = gw_dot(1024, j, 0, HALF)

    def gi_near(j, side):
        gi.near_wait(j, side)
        tile = gi_part[side, j] + gi_dot(1 + side, 1, j, 1, HALF, HALF)
        gi.near(tile, j, side)
        gi.near_start(j, side)

    def gw_near(j):
        for side in range(2):
            gw.near_wait(j, side)
        both = gw_part[j] + gw_dot(1024, j, HALF, HALF)
        for side in range(2):
            gw.near(both[:, side * TILE : (side + 1) * TILE], j, side)
        for side in range(2):
            gw.near_start(j, side)

    def gi_piece(j, k):
        return gi_all.at[:, pl.ds(pl.multiple_of(k * 1024 + j * TILE, TILE), TILE)]

    def gw_piece(i, k):
        return gw_all.at[pl.ds(pl.multiple_of(k * 1024 + i * B, B), B), :]

    def gi_final(j):
        for e in range(2):
            columns = slice(e * 128, (e + 1) * 128)
            gi_fin[j, :, columns] = gi.total(gi_own[j, :, columns], j, e)
        for k in range(4):
            send(gi_fin.at[j, pl.ds(k * 128, 128), :], gi_piece(j, q), gi_fin_send, gi_fin_recv, partner(k))

    def gw_final(j):
        gw_fin_own[...] = gw_own(j)
        for e in range(2):
            columns = slice(e * 128, (e + 1) * 128)
            gw_fin[j, :, columns] = gw.total(gw_fin_own[:, columns], j, e)
            send(
                gw_fin.at[j, :, pl.ds(e * 128, 128)], gw_piece(j // 2, q), gw_fin_send, gw_fin_recv,
                partner(2 * (j % 2) + e),
            )

    def steps_of(count, work, after, name):
        @pl.loop(0, count)
        def _(h):
            with jax.named_scope(name):
                work(h)
            for at, service in after.items():

                @pl.when(h == at)
                def _():
                    with jax.named_scope(name + "_g"):
                        service()

    def forward_4():
        g_first(4)
        g_own(6)
        g_second(3)

    def forward_5():
        g_forward(5)
        g_own(7)
        g_second(4)
        g_first_to_mate(5)

    steps_of(2, lambda h: gi_far_pair(2 * h), {0: forward_4}, "s16_gifar")
    with jax.named_scope("s17_gm23"):
        g_from_mate(2)
        g_from_mate(3)
    steps_of(2, gi_near_part, {0: forward_5}, "s18_gipart")
    with jax.named_scope("s19_trest"):
        t_ring.rest()
        g_from_mate(4)
    steps_of(4, gw_far, {0: lambda: g_first(6), 2: lambda: g_second(5)}, "s20_gwfar")
    with jax.named_scope("s22_gm5"):
        g_from_mate(5)

    @pl.loop(0, 7)
    def _(t):
        @pl.when(t < 4)
        def _():
            with jax.named_scope("s25_giright"):
                gi_near(t, 0)

        @pl.when(t == 0)
        def _():
            with jax.named_scope("s26_g7"):
                g_first(7)

        @pl.when(t == 1)
        def _():
            with jax.named_scope("s24_gm6"):
                g_from_mate(6)

        @pl.when((t > 0) & (t < 5))
        def _():
            with jax.named_scope("s31_gileft"):
                gi_near(t - 1, 1)

        @pl.when(t == 1)
        def _():
            with jax.named_scope("s28_gs7"):
                g_second(7)

        @pl.when(t < 2)
        def _():
            @pl.loop(0, 2)
            def _(k):
                with jax.named_scope("s23_gwpart"):
                    gw_near_part(2 * t + k)

        @pl.when(t == 0)
        def _():
            with jax.named_scope("s27_gs6"):
                g_second(6)

        @pl.when(t > 2)
        def _():
            with jax.named_scope("s35_gifinal"):
                gi_final(t - 3)

        @pl.when(t == 1)
        def _():
            with jax.named_scope("s30_gm7"):
                g_from_mate(7)

        @pl.when((t > 0) & (t < 5))
        def _():
            with jax.named_scope("s33_gwnear"):
                gw_near(t - 1)

        @pl.when(t == 2)
        def _():
            with jax.named_scope("s34_own"):
                gi_own_all()

        @pl.when(t > 2)
        def _():
            with jax.named_scope("s36_gwfinal"):
                gw_final(t - 3)

    with jax.named_scope("s50_drain"):
        for src, sem in ((w_loc, w_ex_send), (tt_loc, t_ex_send), (gi_fin, gi_fin_send), (gw_fin, gw_fin_send)):
            sent_from(src, sem)
        sent_from(g.at[0:B, :], g_ring_send)
        sent_from(g.at[0:B, 0:1024], g_fw_send)
        sent_from(g.at[:, 0:1024], g_mate_send)
        w_ring.drain()
        t_ring.drain()
        gi.drain(sent_from)
        gw.drain(sent_from)
    with jax.named_scope("s52_giout"):
        arrived(gi_all, gi_fin_recv)
    with jax.named_scope("s53_gwout"):
        arrived(gw_all, gw_fin_recv)


def put(gi_from, gw_from, gi_out, gw_out, gi_sem, gw_sem):
    copies = []
    for k in range(4):
        columns, rows = pl.ds(k * 1024, 1024), pl.ds(k * 1024, 1024)
        copies.append(pltpu.make_async_copy(gi_from.at[:, columns], gi_out.at[:, columns], gi_sem.at[k]))
        copies.append(pltpu.make_async_copy(gw_from.at[rows, :], gw_out.at[rows, :], gw_sem.at[k]))
    for copy in copies:
        copy.start()
    for copy in copies:
        copy.wait()


def per_device(tokens, weight, grad_output):
    dma = pltpu.SemaphoreType.DMA
    codes = lambda *lead: pltpu.VMEM((*lead, CODE_ROWS, TILE), BF16)
    any_spec = pl.BlockSpec(memory_space=pl.ANY)
    blocks = pl.pallas_call(
        kernel,
        out_shape=(pltpu.VMEM((128, 4096), BF16), pltpu.VMEM((4096, 128), BF16)),
        in_specs=[any_spec] * 3,
        out_specs=(any_spec, any_spec),
        scratch_shapes=[
            pltpu.VMEM((128, 4096), BF16), pltpu.VMEM((4096, 128), BF16), pltpu.VMEM((4096, 128), BF16),
            pltpu.VMEM((1024, 2048), BF16), pltpu.VMEM((1024, 2048), BF16), pltpu.VMEM((2048, 2048), BF16),
            codes(4), codes(4), codes(2, 4), codes(2, 4), codes(4), codes(4), codes(2, 4), codes(2, 4),
            pltpu.VMEM((4, B, TILE), BF16), pltpu.VMEM((4, B, TILE), BF16), pltpu.VMEM((B, TILE), F32),
            pltpu.VMEM((4, B, TILE), F32), pltpu.VMEM((2, 4, B, TILE), F32), pltpu.VMEM((4, B, 2 * TILE), F32),
            dma(()), dma(()), dma(()),
            dma(()), dma(()), dma((PARTS, 2)), dma((PARTS, 2)),
            dma(()), dma(()), dma(()), dma(()), dma((PARTS, 2)), dma((PARTS, 2)), dma((2,)), dma((2,)),
            dma(()), dma(()), dma(()), dma((8, 3)), dma((8,)),
            dma(()), dma((2, 4)), dma(()), dma((2, 4, 2)), dma(()), dma((2, 4)), dma(()), dma((2, 4, 2)),
            dma(()), dma(()), dma(()), dma(()),
        ],
        compiler_params=pltpu.CompilerParams(
            collective_id=0, has_side_effects=True, vmem_limit_bytes=58 * 1024 * 1024
        ),
        name="linear_backward",
    )(tokens, weight, grad_output)
    return pl.pallas_call(
        put,
        out_shape=tuple(jax.ShapeDtypeStruct(block.shape, BF16) for block in blocks),
        in_specs=[pl.BlockSpec(memory_space=pltpu.VMEM)] * 2,
        out_specs=(any_spec, any_spec),
        scratch_shapes=[dma((4,)), dma((4,))],
        name="put",
    )(*[pltpu.with_memory_space_constraint(block, pltpu.VMEM) for block in blocks])


def solution(mesh):
    return jax.shard_map(
        per_device,
        mesh=mesh,
        in_specs=(P(("row", "col"), "depth"), P("depth", ("col", "row")), P("row", ("col", "depth"))),
        out_specs=(P(("row", "col"), "depth"), P("depth", ("col", "row"))),
        check_vma=False,
    )
```

```python
import jax
import jax.numpy as jnp
from jax import lax
from jax.experimental import pallas as pl
from jax.experimental.pallas import tpu as pltpu
from jax.sharding import PartitionSpec as P

MESH = pl.DeviceIdType.MESH
BF16, F32 = jnp.bfloat16, jnp.float32

B = 512
TILE = 256
CODE_ROWS = B + 8
TOP = 320.0
POWER = 15
PARTS = 4
PART = 1024 // PARTS

OWN, RIGHT, FAR, LEFT = 0, 1, 2, 3
TOKEN_SLOT = {FAR: 0, RIGHT: 1, LEFT: 2, OWN: 3}


def weight_lane(member, pair):
    return {FAR: 0, OWN: 256, RIGHT: 1024, LEFT: 1280}[member] + pair * 512


def token_lane(member, pair):
    return TOKEN_SLOT[member] * B + pair * 256


def encode(tile, ref):
    top = jnp.max(jnp.abs(tile), axis=0, keepdims=True)
    scale = (top * 1.01 + 1e-30).astype(BF16)
    u = tile * (TOP / scale.astype(F32))
    u3 = u * u * u
    u6 = u3 * u3
    ref[0:B, :] = (u6 * u6 * u3).astype(BF16)
    ref[B:CODE_ROWS, :] = jnp.broadcast_to(scale.astype(F32), (8, tile.shape[1])).astype(BF16)


def decode(ref, first=0, rows=B):
    code = ref[first : first + rows, :].astype(F32)
    scale = ref[B:CODE_ROWS, :].astype(F32)[0:1] * (1.0 / TOP)
    size = jnp.exp2(jnp.log2(jnp.abs(code)) * (1.0 / POWER))
    return jnp.where(code < 0, -size, size) * scale


class Reduction:
    def __init__(self, send, arrived, at, far_tx, hop, tx, rx, far_send, hop_recv, send_sem, recv, parts):
        self.send, self.arrived, self.at, self.far_tx, self.hop, self.tx, self.rx = send, arrived, at, far_tx, hop, tx, rx
        self.far_send, self.hop_recv, self.send_sem, self.recv, self.parts = far_send, hop_recv, send_sem, recv, parts

    def half(self, ref, j, side):
        return ref.at[j, :, pl.ds(side * 128, 128)]

    def far(self, tile, j):
        encode(tile, self.far_tx.at[j])

    def far_start(self, j):
        for side in range(2):
            self.send(
                self.half(self.far_tx, j, side), self.half(self.hop, j, side), self.far_send,
                self.hop_recv.at[side, j], self.at(1 + 2 * side),
            )

    def near_wait(self, j, side):
        self.arrived(self.half(self.hop, j, side), self.hop_recv.at[side, j])

    def near(self, tile, j, side):
        parts = [tile[:, 0:128], tile[:, 128:256]]
        parts[side] = parts[side] + decode(self.half(self.hop, j, side))
        encode(jnp.concatenate(parts, axis=1), self.tx.at[side, j])

    def near_start(self, j, side):
        for part, rows in enumerate(self.parts):
            self.send(
                self.tx.at[side, j, rows], self.rx.at[side, j, rows], self.send_sem, self.recv.at[side, j, part],
                self.at(1 + 2 * side),
            )

    def total(self, own, j, part, first, rows):
        for side in range(2):
            self.arrived(self.rx.at[side, j, self.parts[part]], self.recv.at[side, j, part])
        return (own + decode(self.rx.at[0, j], first, rows) + decode(self.rx.at[1, j], first, rows)).astype(BF16)

    def drain(self, sent_from):
        sent_from(self.far_tx, self.far_send)
        sent_from(self.tx, self.send_sem)


def kernel(
    t_hbm, w_hbm, g_hbm, gi_all, gw_all,
    t_loc, w_loc, tt_loc, tt, w, g, gi_far_tx, gi_hop, gi_tx, gi_rx, gw_far_tx, gw_hop, gw_tx, gw_rx, gi_fin, gw_fin, gw_fin_own, gi_own, gi_part, gw_part,
    local_sem, w_local_sem, g_local_sem,
    w_ex_send, t_ex_send, w_ex_recv, t_ex_recv, w_ag_send, t_ag_send, w_fw_send, t_fw_send, w_recv, t_recv, w_rest, t_rest,
    g_ring_send, g_fw_send, g_mate_send, g_recv, g_mate_recv,
    gi_far_send, gi_hop_recv, gi_send, gi_recv, gw_far_send, gw_hop_recv, gw_send, gw_recv,
    gi_fin_send, gi_fin_recv, gw_fin_send, gw_fin_recv,
):
    z, col, yl = lax.axis_index("row"), lax.axis_index("col"), lax.axis_index("depth")
    x, q = col // 4, col % 4
    yh, core = q // 2, q % 2
    y = 2 * yh + yl

    def at_x(k):
        return (z, ((x + k) % 4) * 4 + q, yl)

    def at_z(k):
        return ((z + k) % 4, col, yl)

    def at_y(k):
        other = (y + k) % 4
        return (z, x * 4 + (other // 2) * 2 + core, other % 2)

    mate = (z, x * 4 + yh * 2 + (1 - core), yl)

    def partner(k):
        return (z, x * 4 + k, 1 - yl)

    def send(src, dst, send_sem, recv_sem, to):
        copy = pltpu.make_async_remote_copy(
            src_ref=src, dst_ref=dst, send_sem=send_sem, recv_sem=recv_sem, device_id=to, device_id_type=MESH
        )
        copy.start()

    def arrived(ref, sem):
        pltpu.make_async_remote_copy(
            src_ref=ref, dst_ref=ref, send_sem=sem, recv_sem=sem, device_id=mate, device_id_type=MESH
        ).wait_recv()

    def sent_from(ref, sem):
        pltpu.make_async_remote_copy(
            src_ref=ref, dst_ref=ref, send_sem=sem, recv_sem=sem, device_id=mate, device_id_type=MESH
        ).wait_send()

    steps = ((FAR, 0), (FAR, 1), (RIGHT, 0), (LEFT, 0), (OWN, 0), (RIGHT, 1), (LEFT, 1), (OWN, 1))

    def g_lane(owner, owner_core, late):
        member = (2 * (owner % 2) + (z + late) % 2 - z + 4) % 4
        second = (1 - member // 2) if late == 0 else member // 2
        return pl.multiple_of(late * 1024 + owner_core * 512 + second * 256 + (owner // 2) * 128, 128)

    def g_piece(s, dy, other_core=False, half=None):
        member, late = steps[s]
        start, size = TOKEN_SLOT[member] * B, B
        if half is not None:
            start, size = start + half * (B // 2), B // 2
        lane = g_lane((y + dy) % 4, (1 - core) if other_core else core, late)
        return g.at[pl.ds(start, size), pl.ds(lane, 128)]

    w_copy = pltpu.make_async_copy(w_hbm, w_loc, w_local_sem)
    w_copy.start()
    t_copy = pltpu.make_async_copy(t_hbm, t_loc, local_sem)
    t_copy.start()
    for s, (member, late) in enumerate(steps):
        rows = pl.ds(pl.multiple_of(((x + member) % 4) * B, B), B)
        columns = pl.ds(pl.multiple_of(((z + late) % 2) * 128, 128), 128)
        pltpu.make_async_copy(g_hbm.at[rows, columns], g_piece(s, 0), g_local_sem).start()

    barrier = pltpu.get_barrier_semaphore()
    peers = [at_x(1), at_x(3), at_z(1), at_z(3), mate] + [partner(k) for k in range(4)]
    for peer in peers:
        pl.semaphore_signal(barrier, inc=1, device_id=peer, device_id_type=MESH)
    with jax.named_scope("s00_barrier"):
        pl.semaphore_wait(barrier, len(peers))

    def part_rows(part):
        return pl.ds(part * PART, PART)

    def exchange(src, ref, lane, pair, ex_send, ex_recv, part):
        for k in range(4):
            piece = src.at[pl.ds(k * 1024 + part * PART, PART), :]
            send(piece, ref.at[part_rows(part), pl.ds(lane, 128)], ex_send, ex_recv.at[part, pair], partner(k))

    w_own_lane = pl.multiple_of(core * 512 + 256 + yh * 128, 128)
    t_own_lane = pl.multiple_of(TOKEN_SLOT[OWN] * B + q * 128, 128)
    w_copy.wait()
    exchange(w_loc, w, w_own_lane, core, w_ex_send, w_ex_recv, 0)
    t_copy.wait()
    for k in range(8):
        tt_loc[k * 512 : k * 512 + 512, :] = t_loc[:, k * 512 : k * 512 + 512].T
    exchange(tt_loc, tt, t_own_lane, yh, t_ex_send, t_ex_recv, 0)
    for part in range(1, PARTS):
        exchange(w_loc, w, w_own_lane, core, w_ex_send, w_ex_recv, part)
        exchange(tt_loc, tt, t_own_lane, yh, t_ex_send, t_ex_recv, part)

    def g_own(s):
        piece = g_piece(s, 0)
        send(piece, piece, g_ring_send, g_recv.at[s, 0], at_y(1))
        send(piece, piece, g_ring_send, g_recv.at[s, 1], at_y(3))

    def g_to_mate(s, dy):
        piece = g_piece(s, dy)
        send(piece, piece, g_mate_send, g_mate_recv.at[s], mate)

    def g_forward(s):
        for side, dy in ((0, 3), (1, 1)):
            arrived(g_piece(s, dy), g_recv.at[s, side])
            piece = g_piece(s, dy, half=side)
            send(piece, piece, g_fw_send, g_recv.at[s, 2], at_y(1 + 2 * side))

    def g_first_to_mate(s):
        for dy in (3, 1):
            g_to_mate(s, dy)

    def g_first(s):
        g_forward(s)
        g_first_to_mate(s)

    def g_second(s):
        arrived(g_piece(s, 2), g_recv.at[s, 2])
        g_to_mate(s, 2)

    def g_from_mate(s):
        arrived(g.at[0:B, 0:512], g_mate_recv.at[s])

    pltpu.make_async_copy(tt_loc, tt_loc, g_local_sem).wait()
    g_own(0)
    for s in range(8):
        g_to_mate(s, 0)
    g_own(1)

    class Ring:
        def __init__(self, ref, lane, at, ex_recv, ag_send, fw_send, recv, rest_recv):
            self.ref, self.lane, self.at = ref, lane, at
            self.ex_recv, self.ag_send, self.fw_send, self.recv, self.rest_recv = ex_recv, ag_send, fw_send, recv, rest_recv

        def piece(self, member, part, pair):
            return self.ref.at[part_rows(part), pl.ds(self.lane(member, pair), 256)]

        def own(self, part):
            for pair in range(2):
                piece = self.piece(OWN, part, pair)
                arrived(piece, self.ex_recv.at[part, pair])
                for side, member in ((0, LEFT), (1, RIGHT)):
                    kept = (part < PARTS // 2) == (side == 1)
                    sem = self.rest_recv.at[0] if kept else self.recv.at[part, pair]
                    send(piece, self.piece(member, part, pair), self.ag_send, sem, self.at(1 + 2 * side))

        def forward(self, part):
            side = 0 if part < PARTS // 2 else 1
            for pair in range(2):
                piece = self.piece((LEFT, RIGHT)[side], part, pair)
                arrived(piece, self.recv.at[part, pair])
                send(piece, self.piece(FAR, part, pair), self.fw_send, self.rest_recv.at[1], self.at(1 + 2 * side))

        def rest(self):
            for k in range(2):
                arrived(self.ref.at[:, 0:512], self.rest_recv.at[k])

        def drain(self):
            sent_from(self.ref.at[:, 0:1024], self.ag_send)
            sent_from(self.ref.at[:, 0:512], self.fw_send)

    w_ring = Ring(w, weight_lane, at_z, w_ex_recv, w_ag_send, w_fw_send, w_recv, w_rest)
    t_ring = Ring(tt, token_lane, at_x, t_ex_recv, t_ag_send, t_fw_send, t_recv, t_rest)

    with jax.named_scope("s02_own01"):
        w_ring.own(0)
        t_ring.own(0)
        w_ring.own(1)
    with jax.named_scope("s03_own12"):
        t_ring.own(1)
        w_ring.forward(0)
        w_ring.own(2)
        t_ring.forward(0)
        t_ring.own(2)
    with jax.named_scope("s04_own3"):
        w_ring.forward(1)
        w_ring.own(3)
        t_ring.forward(1)
        t_ring.own(3)
    with jax.named_scope("s05_wfw2"):
        w_ring.forward(2)
    with jax.named_scope("s08_g0"):
        g_first(0)
        g_own(2)
    with jax.named_scope("s09_tfw2wfw3"):
        t_ring.forward(2)
        w_ring.forward(3)
    with jax.named_scope("s10_g1"):
        g_first(1)
        g_own(3)
        g_second(0)
    with jax.named_scope("s11_tfw3"):
        t_ring.forward(3)
    with jax.named_scope("s12_g2"):
        g_first(2)
        g_own(4)
        g_second(1)
    with jax.named_scope("s13_g3"):
        g_first(3)
        g_own(5)
        g_second(2)
    with jax.named_scope("s14_wrest"):
        w_ring.rest()
    with jax.named_scope("s15_gm01"):
        g_from_mate(0)
        g_from_mate(1)

    by_rows = (((1,), (1,)), ((), ()))

    HALF = 1024

    def gi_dot(slot, slots, j, tiles, first=0, terms=2 * HALF):
        return lax.dot_general(
            g[slot * B : (slot + slots) * B, first : first + terms],
            w[pl.ds(pl.multiple_of(j * TILE, TILE), tiles * TILE), first : first + terms],
            by_rows, preferred_element_type=F32,
        )

    def gw_dot(lane, j, first=0, terms=2 * HALF):
        rows = pl.ds(pl.multiple_of((j // 2) * B, B), B)
        columns = pl.ds(pl.multiple_of(lane + (j % 2) * 512, 512), 512)
        return jnp.dot(tt[rows, first : first + terms], g[first : first + terms, columns], preferred_element_type=F32)

    whole, in_two = (pl.ds(0, CODE_ROWS),), (pl.ds(B // 2, CODE_ROWS - B // 2), pl.ds(0, B // 2))
    gi = Reduction(send, arrived, at_x, gi_far_tx, gi_hop, gi_tx, gi_rx, gi_far_send, gi_hop_recv, gi_send, gi_recv, whole)
    gw = Reduction(send, arrived, at_z, gw_far_tx, gw_hop, gw_tx, gw_rx, gw_far_send, gw_hop_recv, gw_send, gw_recv, in_two)

    def gi_far_pair(j):
        both = gi_dot(0, 1, j, 2)
        for k in range(2):
            gi.far(both[:, k * TILE : (k + 1) * TILE], j + k)
        for k in range(2):
            gi.far_start(j + k)

    def gw_far(t):
        j = 2 * (t % 2) + t // 2
        rows = pl.ds(pl.multiple_of((t % 2) * B, B), B)
        columns = pl.ds(pl.multiple_of((t // 2) * 512, 512), TILE)
        gw.far(jnp.dot(tt[rows, :], g[:, columns], preferred_element_type=F32), j)
        gw.far_start(j)

    def gw_own(j):
        rows = pl.ds(pl.multiple_of((j // 2) * B, B), B)
        columns = pl.ds(pl.multiple_of((j % 2) * 512 + TILE, TILE), TILE)
        return jnp.dot(tt[rows, :], g[:, columns], preferred_element_type=F32)

    def gi_near_part(h):
        both = gi_dot(1, 2, 2 * h, 2, 0, HALF)
        for side in range(2):
            for k in range(2):
                gi_part[side, 2 * h + k] = both[side * B : (side + 1) * B, k * TILE : (k + 1) * TILE]

    def gi_own_terms(first):
        @pl.loop(0, 2)
        def _(h):
            both = gi_dot(3, 1, 2 * h, 2, first, HALF)
            for k in range(2):
                terms = both[:, k * TILE : (k + 1) * TILE]
                gi_own[2 * h + k] = terms if first == 0 else gi_own[2 * h + k] + terms

    def gw_near_part(j):
        gw_part[j] = gw_dot(1024, j, 0, HALF)

    def gi_near(j, side):
        gi.near_wait(j, side)
        tile = gi_part[side, j] + gi_dot(1 + side, 1, j, 1, HALF, HALF)
        gi.near(tile, j, side)
        gi.near_start(j, side)

    def gw_near(j):
        for side in range(2):
            gw.near_wait(j, side)
        both = gw_part[j] + gw_dot(1024, j, HALF, HALF)
        for side in range(2):
            gw.near(both[:, side * TILE : (side + 1) * TILE], j, side)
        for side in range(2):
            gw.near_start(j, side)

    def gi_piece(j, k):
        return gi_all.at[:, pl.ds(pl.multiple_of(k * 1024 + j * TILE, TILE), TILE)]

    def gw_piece(i, first):
        return gw_all.at[pl.ds(pl.multiple_of(q * 1024 + i * B + first, B // 2), B // 2), :]

    def gi_final(j):
        gi_fin[j] = gi.total(gi_own[j], j, 0, 0, B)
        for k in range(4):
            send(gi_fin.at[j, pl.ds(k * 128, 128), :], gi_piece(j, q), gi_fin_send, gi_fin_recv, partner(k))

    def gw_final(j):
        gw_fin_own[...] = gw_own(j)
        for part, first in enumerate((B // 2, 0)):
            rows = slice(first, first + B // 2)
            gw_fin[j, rows, :] = gw.total(gw_fin_own[rows, :], j, part, first, B // 2)
            for e in range(2):
                send(
                    gw_fin.at[j, pl.ds(first, B // 2), pl.ds(e * 128, 128)], gw_piece(j // 2, first), gw_fin_send,
                    gw_fin_recv, partner(j % 2 + 2 * e),
                )

    def steps_of(count, work, after, name):
        @pl.loop(0, count)
        def _(h):
            with jax.named_scope(name):
                work(h)
            for at, service in after.items():

                @pl.when(h == at)
                def _():
                    with jax.named_scope(name + "_g"):
                        service()

    def forward_4():
        g_first(4)
        g_own(6)
        g_second(3)

    def forward_5():
        g_forward(5)
        g_own(7)
        g_second(4)
        g_first_to_mate(5)

    steps_of(2, lambda h: gi_far_pair(2 * h), {0: forward_4}, "s16_gifar")
    with jax.named_scope("s17_gm23"):
        g_from_mate(2)
        g_from_mate(3)
    steps_of(2, gi_near_part, {0: forward_5}, "s18_gipart")
    with jax.named_scope("s19_trest"):
        t_ring.rest()
        g_from_mate(4)
    steps_of(4, gw_far, {0: lambda: g_first(6), 2: lambda: g_second(5)}, "s20_gwfar")
    with jax.named_scope("s22_gm5"):
        g_from_mate(5)

    with jax.named_scope("s25_giright0"):
        gi_near(0, 0)
    with jax.named_scope("s26_g7"):
        g_first(7)

    @pl.loop(0, 2)
    def _(j):
        with jax.named_scope("s27_gwpart"):
            gw_near_part(j)

    with jax.named_scope("s28_gs6"):
        g_second(6)
    with jax.named_scope("s29_giright1"):
        gi_near(1, 0)
    with jax.named_scope("s30_gm6"):
        g_from_mate(6)

    @pl.loop(0, 5)
    def _(u):
        @pl.when(u < 4)
        def _():
            with jax.named_scope("s31_gileft"):
                gi_near(u, 1)

        @pl.when(u == 0)
        def _():
            with jax.named_scope("s32_gs7"):
                g_second(7)

        for at in range(2):

            @pl.when(u == at)
            def _():
                with jax.named_scope("s33_giown"):
                    gi_own_terms(at * HALF)

        @pl.when(u == 0)
        def _():
            with jax.named_scope("s34_gm7"):
                g_from_mate(7)

        @pl.when(u < 4)
        def _():
            with jax.named_scope("s35_gwnear"):
                gw_near(u)

        @pl.when(u > 0)
        def _():
            with jax.named_scope("s36_gifinal"):
                gi_final(u - 1)

        @pl.when(u < 2)
        def _():
            with jax.named_scope("s37_giright"):
                gi_near(u + 2, 0)
            with jax.named_scope("s38_gwpart"):
                gw_near_part(u + 2)

        @pl.when(u > 0)
        def _():
            with jax.named_scope("s39_gwfinal"):
                gw_final(u - 1)

    with jax.named_scope("s50_drain"):
        for src, sem in ((w_loc, w_ex_send), (tt_loc, t_ex_send), (gi_fin, gi_fin_send), (gw_fin, gw_fin_send)):
            sent_from(src, sem)
        sent_from(g.at[0:B, :], g_ring_send)
        sent_from(g.at[0:B, 0:1024], g_fw_send)
        sent_from(g.at[:, 0:1024], g_mate_send)
        w_ring.drain()
        t_ring.drain()
        gi.drain(sent_from)
        gw.drain(sent_from)
    with jax.named_scope("s52_giout"):
        arrived(gi_all, gi_fin_recv)
    with jax.named_scope("s53_gwout"):
        arrived(gw_all, gw_fin_recv)


def put(gi_from, gw_from, gi_out, gw_out, gi_sem, gw_sem):
    copies = []
    for k in range(4):
        columns, rows = pl.ds(k * 1024, 1024), pl.ds(k * 1024, 1024)
        copies.append(pltpu.make_async_copy(gi_from.at[:, columns], gi_out.at[:, columns], gi_sem.at[k]))
        copies.append(pltpu.make_async_copy(gw_from.at[rows, :], gw_out.at[rows, :], gw_sem.at[k]))
    for copy in copies:
        copy.start()
    for copy in copies:
        copy.wait()


def per_device(tokens, weight, grad_output):
    dma = pltpu.SemaphoreType.DMA
    codes = lambda *lead: pltpu.VMEM((*lead, CODE_ROWS, TILE), BF16)
    any_spec = pl.BlockSpec(memory_space=pl.ANY)
    blocks = pl.pallas_call(
        kernel,
        out_shape=(pltpu.VMEM((128, 4096), BF16), pltpu.VMEM((4096, 128), BF16)),
        in_specs=[any_spec] * 3,
        out_specs=(any_spec, any_spec),
        scratch_shapes=[
            pltpu.VMEM((128, 4096), BF16), pltpu.VMEM((4096, 128), BF16), pltpu.VMEM((4096, 128), BF16),
            pltpu.VMEM((1024, 2048), BF16), pltpu.VMEM((1024, 2048), BF16), pltpu.VMEM((2048, 2048), BF16),
            codes(4), codes(4), codes(2, 4), codes(2, 4), codes(4), codes(4), codes(2, 4), codes(2, 4),
            pltpu.VMEM((4, B, TILE), BF16), pltpu.VMEM((4, B, TILE), BF16), pltpu.VMEM((B, TILE), F32),
            pltpu.VMEM((4, B, TILE), F32), pltpu.VMEM((2, 4, B, TILE), F32), pltpu.VMEM((4, B, 2 * TILE), F32),
            dma(()), dma(()), dma(()),
            dma(()), dma(()), dma((PARTS, 2)), dma((PARTS, 2)),
            dma(()), dma(()), dma(()), dma(()), dma((PARTS, 2)), dma((PARTS, 2)), dma((2,)), dma((2,)),
            dma(()), dma(()), dma(()), dma((8, 3)), dma((8,)),
            dma(()), dma((2, 4)), dma(()), dma((2, 4, 1)), dma(()), dma((2, 4)), dma(()), dma((2, 4, 2)),
            dma(()), dma(()), dma(()), dma(()),
        ],
        compiler_params=pltpu.CompilerParams(
            collective_id=0, has_side_effects=True, vmem_limit_bytes=58 * 1024 * 1024
        ),
        name="linear_backward",
    )(tokens, weight, grad_output)
    return pl.pallas_call(
        put,
        out_shape=tuple(jax.ShapeDtypeStruct(block.shape, BF16) for block in blocks),
        in_specs=[pl.BlockSpec(memory_space=pltpu.VMEM)] * 2,
        out_specs=(any_spec, any_spec),
        scratch_shapes=[dma((4,)), dma((4,))],
        name="put",
    )(*[pltpu.with_memory_space_constraint(block, pltpu.VMEM) for block in blocks])


def solution(mesh):
    return jax.shard_map(
        per_device,
        mesh=mesh,
        in_specs=(P(("row", "col"), "depth"), P("depth", ("col", "row")), P("row", ("col", "depth"))),
        out_specs=(P(("row", "col"), "depth"), P("depth", ("col", "row"))),
        check_vma=False,
    )
```

```python
import jax
import jax.numpy as jnp
from jax import lax
from jax.experimental import pallas as pl
from jax.experimental.pallas import tpu as pltpu
from jax.sharding import PartitionSpec as P

MESH = pl.DeviceIdType.MESH
BF16, F32 = jnp.bfloat16, jnp.float32

B = 512
TILE = 256
CODE_ROWS = B + 8
TOP = 320.0
POWER = 15
PARTS = 4
PART = 1024 // PARTS

OWN, RIGHT, FAR, LEFT = 0, 1, 2, 3
TOKEN_SLOT = {FAR: 0, RIGHT: 1, LEFT: 2, OWN: 3}


def weight_lane(member, pair):
    return {FAR: 0, OWN: 256, RIGHT: 1024, LEFT: 1280}[member] + pair * 512


def token_lane(member, pair):
    return TOKEN_SLOT[member] * B + pair * 256


def encode(tile, ref):
    top = jnp.max(jnp.abs(tile), axis=0, keepdims=True)
    scale = (top * 1.01 + 1e-30).astype(BF16)
    u = tile * (TOP / scale.astype(F32))
    u3 = u * u * u
    u6 = u3 * u3
    ref[0:B, :] = (u6 * u6 * u3).astype(BF16)
    ref[B:CODE_ROWS, :] = jnp.broadcast_to(scale.astype(F32), (8, tile.shape[1])).astype(BF16)


def decode(ref, first=0, rows=B):
    code = ref[first : first + rows, :].astype(F32)
    scale = ref[B:CODE_ROWS, :].astype(F32)[0:1] * (1.0 / TOP)
    size = jnp.exp2(jnp.log2(jnp.abs(code)) * (1.0 / POWER))
    return jnp.where(code < 0, -size, size) * scale


class Reduction:
    def __init__(self, send, arrived, at, far_tx, hop, tx, rx, far_send, hop_recv, send_sem, recv, parts):
        self.send, self.arrived, self.at, self.far_tx, self.hop, self.tx, self.rx = send, arrived, at, far_tx, hop, tx, rx
        self.far_send, self.hop_recv, self.send_sem, self.recv, self.parts = far_send, hop_recv, send_sem, recv, parts

    def half(self, ref, j, side):
        return ref.at[j, :, pl.ds(side * 128, 128)]

    def far(self, tile, j):
        encode(tile, self.far_tx.at[j])

    def far_start(self, j):
        for side in range(2):
            self.send(
                self.half(self.far_tx, j, side), self.half(self.hop, j, side), self.far_send,
                self.hop_recv.at[side, j], self.at(1 + 2 * side),
            )

    def near_wait(self, j, side):
        self.arrived(self.half(self.hop, j, side), self.hop_recv.at[side, j])

    def near(self, tile, j, side):
        parts = [tile[:, 0:128], tile[:, 128:256]]
        parts[side] = parts[side] + decode(self.half(self.hop, j, side))
        encode(jnp.concatenate(parts, axis=1), self.tx.at[side, j])

    def near_start(self, j, side):
        for part, rows in enumerate(self.parts):
            self.send(
                self.tx.at[side, j, rows], self.rx.at[side, j, rows], self.send_sem, self.recv.at[j, part],
                self.at(1 + 2 * side),
            )

    def total(self, own, j, part, first, rows):
        self.arrived(self.rx.at[:, j, self.parts[part]], self.recv.at[j, part])
        return (own + decode(self.rx.at[0, j], first, rows) + decode(self.rx.at[1, j], first, rows)).astype(BF16)

    def drain(self, sent_from):
        sent_from(self.far_tx, self.far_send)
        sent_from(self.tx, self.send_sem)


def kernel(
    t_hbm, w_hbm, g_hbm, gi_all, gw_all,
    t_loc, w_loc, tt_loc, tt, w, g, gi_far_tx, gi_hop, gi_tx, gi_rx, gw_far_tx, gw_hop, gw_tx, gw_rx, gi_fin, gw_fin, gw_fin_own, gi_own, gi_part, gw_part,
    local_sem, w_local_sem, g_local_sem,
    w_ex_send, t_ex_send, w_ex_recv, t_ex_recv, w_ag_send, t_ag_send, w_fw_send, t_fw_send, w_recv, t_recv, w_rest, t_rest,
    g_ring_send, g_fw_send, g_mate_send, g_recv, g_mate_recv,
    gi_far_send, gi_hop_recv, gi_send, gi_recv, gw_far_send, gw_hop_recv, gw_send, gw_recv,
    gi_fin_send, gi_fin_recv, gw_fin_send, gw_fin_recv,
):
    z, col, yl = lax.axis_index("row"), lax.axis_index("col"), lax.axis_index("depth")
    x, q = col // 4, col % 4
    yh, core = q // 2, q % 2
    y = 2 * yh + yl

    def at_x(k):
        return (z, ((x + k) % 4) * 4 + q, yl)

    def at_z(k):
        return ((z + k) % 4, col, yl)

    def at_y(k):
        other = (y + k) % 4
        return (z, x * 4 + (other // 2) * 2 + core, other % 2)

    mate = (z, x * 4 + yh * 2 + (1 - core), yl)

    def partner(k):
        return (z, x * 4 + k, 1 - yl)

    def send(src, dst, send_sem, recv_sem, to):
        copy = pltpu.make_async_remote_copy(
            src_ref=src, dst_ref=dst, send_sem=send_sem, recv_sem=recv_sem, device_id=to, device_id_type=MESH
        )
        copy.start()

    def arrived(ref, sem):
        pltpu.make_async_remote_copy(
            src_ref=ref, dst_ref=ref, send_sem=sem, recv_sem=sem, device_id=mate, device_id_type=MESH
        ).wait_recv()

    def sent_from(ref, sem):
        pltpu.make_async_remote_copy(
            src_ref=ref, dst_ref=ref, send_sem=sem, recv_sem=sem, device_id=mate, device_id_type=MESH
        ).wait_send()

    steps = ((FAR, 0), (FAR, 1), (RIGHT, 0), (LEFT, 0), (OWN, 0), (RIGHT, 1), (LEFT, 1), (OWN, 1))

    def g_lane(owner, owner_core, late):
        member = (2 * (owner % 2) + (z + late) % 2 - z + 4) % 4
        second = (1 - member // 2) if late == 0 else member // 2
        return pl.multiple_of(late * 1024 + owner_core * 512 + second * 256 + (owner // 2) * 128, 128)

    def g_piece(s, dy, other_core=False, half=None):
        member, late = steps[s]
        start, size = TOKEN_SLOT[member] * B, B
        if half is not None:
            start, size = start + half * (B // 2), B // 2
        lane = g_lane((y + dy) % 4, (1 - core) if other_core else core, late)
        return g.at[pl.ds(start, size), pl.ds(lane, 128)]

    w_copy = pltpu.make_async_copy(w_hbm, w_loc, w_local_sem)
    w_copy.start()
    t_copy = pltpu.make_async_copy(t_hbm, t_loc, local_sem)
    t_copy.start()
    for s, (member, late) in enumerate(steps):
        rows = pl.ds(pl.multiple_of(((x + member) % 4) * B, B), B)
        columns = pl.ds(pl.multiple_of(((z + late) % 2) * 128, 128), 128)
        pltpu.make_async_copy(g_hbm.at[rows, columns], g_piece(s, 0), g_local_sem).start()

    barrier = pltpu.get_barrier_semaphore()
    peers = [at_x(1), at_x(3), at_z(1), at_z(3), mate] + [partner(k) for k in range(4)]
    for peer in peers:
        pl.semaphore_signal(barrier, inc=1, device_id=peer, device_id_type=MESH)
    with jax.named_scope("s00_barrier"):
        pl.semaphore_wait(barrier, len(peers))

    def part_rows(part):
        return pl.ds(part * PART, PART)

    def exchange(src, ref, lane, ex_send, ex_recv, part):
        for k in range(4):
            piece = src.at[pl.ds(k * 1024 + part * PART, PART), :]
            send(piece, ref.at[part_rows(part), pl.ds(lane, 128)], ex_send, ex_recv.at[part], partner(k))

    w_own_lane = pl.multiple_of(core * 512 + 256 + yh * 128, 128)
    t_own_lane = pl.multiple_of(TOKEN_SLOT[OWN] * B + q * 128, 128)
    w_copy.wait()
    exchange(w_loc, w, w_own_lane, w_ex_send, w_ex_recv, 0)
    t_copy.wait()
    for k in range(8):
        tt_loc[k * 512 : k * 512 + 512, :] = t_loc[:, k * 512 : k * 512 + 512].T
    exchange(tt_loc, tt, t_own_lane, t_ex_send, t_ex_recv, 0)
    for part in range(1, PARTS):
        exchange(w_loc, w, w_own_lane, w_ex_send, w_ex_recv, part)
        exchange(tt_loc, tt, t_own_lane, t_ex_send, t_ex_recv, part)

    def g_own(s):
        piece = g_piece(s, 0)
        send(piece, piece, g_ring_send, g_recv.at[s, 0], at_y(1))
        send(piece, piece, g_ring_send, g_recv.at[s, 1], at_y(3))

    def g_to_mate(s, dy):
        piece = g_piece(s, dy)
        send(piece, piece, g_mate_send, g_mate_recv.at[s], mate)

    def g_forward(s):
        for side, dy in ((0, 3), (1, 1)):
            arrived(g_piece(s, dy), g_recv.at[s, side])
            piece = g_piece(s, dy, half=side)
            send(piece, piece, g_fw_send, g_recv.at[s, 2], at_y(1 + 2 * side))

    def g_first_to_mate(s):
        for dy in (3, 1):
            g_to_mate(s, dy)

    def g_first(s):
        g_forward(s)
        g_first_to_mate(s)

    def g_second(s):
        arrived(g_piece(s, 2), g_recv.at[s, 2])
        g_to_mate(s, 2)

    def g_from_mate(s):
        arrived(g.at[0:B, 0:512], g_mate_recv.at[s])

    pltpu.make_async_copy(tt_loc, tt_loc, g_local_sem).wait()
    g_own(0)
    for s in range(8):
        g_to_mate(s, 0)
    g_own(1)

    class Ring:
        def __init__(self, ref, lane, at, ex_recv, ag_send, fw_send, recv, rest_recv):
            self.ref, self.lane, self.at = ref, lane, at
            self.ex_recv, self.ag_send, self.fw_send, self.recv, self.rest_recv = ex_recv, ag_send, fw_send, recv, rest_recv

        def piece(self, member, part, pair):
            return self.ref.at[part_rows(part), pl.ds(self.lane(member, pair), 256)]

        def own(self, part):
            arrived(self.ref.at[part_rows(part), 0:512], self.ex_recv.at[part])
            for pair in range(2):
                piece = self.piece(OWN, part, pair)
                for side, member in ((0, LEFT), (1, RIGHT)):
                    kept = (part < PARTS // 2) == (side == 1)
                    sem = self.rest_recv.at[0] if kept else self.recv.at[part, pair]
                    send(piece, self.piece(member, part, pair), self.ag_send, sem, self.at(1 + 2 * side))

        def forward(self, part):
            side = 0 if part < PARTS // 2 else 1
            for pair in range(2):
                piece = self.piece((LEFT, RIGHT)[side], part, pair)
                arrived(piece, self.recv.at[part, pair])
                send(piece, self.piece(FAR, part, pair), self.fw_send, self.rest_recv.at[1], self.at(1 + 2 * side))

        def rest(self):
            for k in range(2):
                arrived(self.ref.at[:, 0:512], self.rest_recv.at[k])

        def drain(self):
            sent_from(self.ref.at[:, 0:1024], self.ag_send)
            sent_from(self.ref.at[:, 0:512], self.fw_send)

    w_ring = Ring(w, weight_lane, at_z, w_ex_recv, w_ag_send, w_fw_send, w_recv, w_rest)
    t_ring = Ring(tt, token_lane, at_x, t_ex_recv, t_ag_send, t_fw_send, t_recv, t_rest)

    with jax.named_scope("s02_own01"):
        w_ring.own(0)
        t_ring.own(0)
        w_ring.own(1)
    with jax.named_scope("s03_own12"):
        t_ring.own(1)
        w_ring.forward(0)
        w_ring.own(2)
        t_ring.forward(0)
        t_ring.own(2)
    with jax.named_scope("s04_own3"):
        w_ring.forward(1)
        w_ring.own(3)
        t_ring.forward(1)
        t_ring.own(3)
    with jax.named_scope("s05_wfw2"):
        w_ring.forward(2)
    with jax.named_scope("s08_g0"):
        g_first(0)
        g_own(2)
    with jax.named_scope("s09_tfw2wfw3"):
        t_ring.forward(2)
        w_ring.forward(3)
    with jax.named_scope("s10_g1"):
        g_first(1)
        g_own(3)
        g_second(0)
    with jax.named_scope("s11_tfw3"):
        t_ring.forward(3)
    with jax.named_scope("s12_g2"):
        g_first(2)
        g_own(4)
        g_second(1)
    with jax.named_scope("s13_g3"):
        g_first(3)
        g_own(5)
        g_second(2)
    with jax.named_scope("s14_wrest"):
        w_ring.rest()
    with jax.named_scope("s15_gm01"):
        g_from_mate(0)
        g_from_mate(1)

    by_rows = (((1,), (1,)), ((), ()))

    HALF = 1024

    def gi_dot(slot, slots, j, tiles, first=0, terms=2 * HALF):
        return lax.dot_general(
            g[slot * B : (slot + slots) * B, first : first + terms],
            w[pl.ds(pl.multiple_of(j * TILE, TILE), tiles * TILE), first : first + terms],
            by_rows, preferred_element_type=F32,
        )

    def gw_dot(lane, j, first=0, terms=2 * HALF):
        rows = pl.ds(pl.multiple_of((j // 2) * B, B), B)
        columns = pl.ds(pl.multiple_of(lane + (j % 2) * 512, 512), 512)
        return jnp.dot(tt[rows, first : first + terms], g[first : first + terms, columns], preferred_element_type=F32)

    whole, in_two = (pl.ds(0, CODE_ROWS),), (pl.ds(B // 2, CODE_ROWS - B // 2), pl.ds(0, B // 2))
    gi = Reduction(send, arrived, at_x, gi_far_tx, gi_hop, gi_tx, gi_rx, gi_far_send, gi_hop_recv, gi_send, gi_recv, whole)
    gw = Reduction(send, arrived, at_z, gw_far_tx, gw_hop, gw_tx, gw_rx, gw_far_send, gw_hop_recv, gw_send, gw_recv, in_two)

    def gi_far_pair(j):
        both = gi_dot(0, 1, j, 2)
        for k in range(2):
            gi.far(both[:, k * TILE : (k + 1) * TILE], j + k)
        for k in range(2):
            gi.far_start(j + k)

    def gw_far(t):
        j = 2 * (t % 2) + t // 2
        rows = pl.ds(pl.multiple_of((t % 2) * B, B), B)
        columns = pl.ds(pl.multiple_of((t // 2) * 512, 512), TILE)
        gw.far(jnp.dot(tt[rows, :], g[:, columns], preferred_element_type=F32), j)
        gw.far_start(j)

    def gw_own(j):
        rows = pl.ds(pl.multiple_of((j // 2) * B, B), B)
        columns = pl.ds(pl.multiple_of((j % 2) * 512 + TILE, TILE), TILE)
        return jnp.dot(tt[rows, :], g[:, columns], preferred_element_type=F32)

    def gi_near_part(h):
        both = gi_dot(1, 2, 2 * h, 2, 0, HALF)
        for side in range(2):
            for k in range(2):
                gi_part[side, 2 * h + k] = both[side * B : (side + 1) * B, k * TILE : (k + 1) * TILE]

    def gi_own_terms(first):
        @pl.loop(0, 2)
        def _(h):
            both = gi_dot(3, 1, 2 * h, 2, first, HALF)
            for k in range(2):
                terms = both[:, k * TILE : (k + 1) * TILE]
                gi_own[2 * h + k] = terms if first == 0 else gi_own[2 * h + k] + terms

    def gw_near_part(j):
        gw_part[j] = gw_dot(1024, j, 0, HALF)

    def gi_near(j, side):
        gi.near_wait(j, side)
        tile = gi_part[side, j] + gi_dot(1 + side, 1, j, 1, HALF, HALF)
        gi.near(tile, j, side)
        gi.near_start(j, side)

    def gw_near(j):
        for side in range(2):
            gw.near_wait(j, side)
        both = gw_part[j] + gw_dot(1024, j, HALF, HALF)
        for side in range(2):
            gw.near(both[:, side * TILE : (side + 1) * TILE], j, side)
        for side in range(2):
            gw.near_start(j, side)

    def gi_piece(j, k):
        return gi_all.at[:, pl.ds(pl.multiple_of(k * 1024 + j * TILE, TILE), TILE)]

    def gw_piece(i, first):
        return gw_all.at[pl.ds(pl.multiple_of(q * 1024 + i * B + first, B // 2), B // 2), :]

    def gi_final(j):
        gi_fin[j] = gi.total(gi_own[j], j, 0, 0, B)
        for k in range(4):
            send(gi_fin.at[j, pl.ds(k * 128, 128), :], gi_piece(j, q), gi_fin_send, gi_fin_recv, partner(k))

    def gw_final(j):
        gw_fin_own[...] = gw_own(j)
        for part, first in enumerate((B // 2, 0)):
            rows = slice(first, first + B // 2)
            gw_fin[j, rows, :] = gw.total(gw_fin_own[rows, :], j, part, first, B // 2)
            for e in range(2):
                send(
                    gw_fin.at[j, pl.ds(first, B // 2), pl.ds(e * 128, 128)], gw_piece(j // 2, first), gw_fin_send,
                    gw_fin_recv, partner(j % 2 + 2 * e),
                )

    def steps_of(count, work, after, name):
        @pl.loop(0, count)
        def _(h):
            with jax.named_scope(name):
                work(h)
            for at, service in after.items():

                @pl.when(h == at)
                def _():
                    with jax.named_scope(name + "_g"):
                        service()

    def forward_4():
        g_first(4)
        g_own(6)
        g_second(3)

    def forward_5():
        g_forward(5)
        g_own(7)
        g_second(4)
        g_first_to_mate(5)

    steps_of(2, lambda h: gi_far_pair(2 * h), {0: forward_4}, "s16_gifar")
    with jax.named_scope("s17_gm23"):
        g_from_mate(2)
        g_from_mate(3)
    steps_of(2, gi_near_part, {0: forward_5}, "s18_gipart")
    with jax.named_scope("s19_trest"):
        t_ring.rest()
        g_from_mate(4)
    steps_of(4, gw_far, {0: lambda: g_first(6), 2: lambda: g_second(5)}, "s20_gwfar")
    with jax.named_scope("s22_gm5"):
        g_from_mate(5)

    with jax.named_scope("s25_giright0"):
        gi_near(0, 0)
    with jax.named_scope("s26_g7"):
        g_first(7)

    @pl.loop(0, 2)
    def _(j):
        with jax.named_scope("s27_gwpart"):
            gw_near_part(j)

    with jax.named_scope("s28_gs6"):
        g_second(6)
    with jax.named_scope("s29_giright1"):
        gi_near(1, 0)
    with jax.named_scope("s30_gm6"):
        g_from_mate(6)

    @pl.loop(0, 5)
    def _(u):
        @pl.when(u < 4)
        def _():
            with jax.named_scope("s31_gileft"):
                gi_near(u, 1)

        @pl.when(u == 0)
        def _():
            with jax.named_scope("s32_gs7"):
                g_second(7)

        for at in range(2):

            @pl.when(u == at)
            def _():
                with jax.named_scope("s33_giown"):
                    gi_own_terms(at * HALF)

        @pl.when(u == 0)
        def _():
            with jax.named_scope("s34_gm7"):
                g_from_mate(7)

        @pl.when(u < 4)
        def _():
            with jax.named_scope("s35_gwnear"):
                gw_near(u)

        @pl.when(u > 0)
        def _():
            with jax.named_scope("s36_gifinal"):
                gi_final(u - 1)

        @pl.when(u < 2)
        def _():
            with jax.named_scope("s37_giright"):
                gi_near(u + 2, 0)
            with jax.named_scope("s38_gwpart"):
                gw_near_part(u + 2)

        @pl.when(u > 0)
        def _():
            with jax.named_scope("s39_gwfinal"):
                gw_final(u - 1)

    with jax.named_scope("s50_drain"):
        for src, sem in ((w_loc, w_ex_send), (tt_loc, t_ex_send), (gi_fin, gi_fin_send), (gw_fin, gw_fin_send)):
            sent_from(src, sem)
        sent_from(g.at[0:B, :], g_ring_send)
        sent_from(g.at[0:B, 0:1024], g_fw_send)
        sent_from(g.at[:, 0:1024], g_mate_send)
        w_ring.drain()
        t_ring.drain()
        gi.drain(sent_from)
        gw.drain(sent_from)
    with jax.named_scope("s52_giout"):
        arrived(gi_all, gi_fin_recv)
    with jax.named_scope("s53_gwout"):
        arrived(gw_all, gw_fin_recv)


def put(gi_from, gw_from, gi_out, gw_out, gi_sem, gw_sem):
    copies = []
    for k in range(4):
        columns, rows = pl.ds(k * 1024, 1024), pl.ds(k * 1024, 1024)
        copies.append(pltpu.make_async_copy(gi_from.at[:, columns], gi_out.at[:, columns], gi_sem.at[k]))
        copies.append(pltpu.make_async_copy(gw_from.at[rows, :], gw_out.at[rows, :], gw_sem.at[k]))
    for copy in copies:
        copy.start()
    for copy in copies:
        copy.wait()


def per_device(tokens, weight, grad_output):
    dma = pltpu.SemaphoreType.DMA
    codes = lambda *lead: pltpu.VMEM((*lead, CODE_ROWS, TILE), BF16)
    any_spec = pl.BlockSpec(memory_space=pl.ANY)
    blocks = pl.pallas_call(
        kernel,
        out_shape=(pltpu.VMEM((128, 4096), BF16), pltpu.VMEM((4096, 128), BF16)),
        in_specs=[any_spec] * 3,
        out_specs=(any_spec, any_spec),
        scratch_shapes=[
            pltpu.VMEM((128, 4096), BF16), pltpu.VMEM((4096, 128), BF16), pltpu.VMEM((4096, 128), BF16),
            pltpu.VMEM((1024, 2048), BF16), pltpu.VMEM((1024, 2048), BF16), pltpu.VMEM((2048, 2048), BF16),
            codes(4), codes(4), codes(2, 4), codes(2, 4), codes(4), codes(4), codes(2, 4), codes(2, 4),
            pltpu.VMEM((4, B, TILE), BF16), pltpu.VMEM((4, B, TILE), BF16), pltpu.VMEM((B, TILE), F32),
            pltpu.VMEM((4, B, TILE), F32), pltpu.VMEM((2, 4, B, TILE), F32), pltpu.VMEM((4, B, 2 * TILE), F32),
            dma(()), dma(()), dma(()),
            dma(()), dma(()), dma((PARTS,)), dma((PARTS,)),
            dma(()), dma(()), dma(()), dma(()), dma((PARTS, 2)), dma((PARTS, 2)), dma((2,)), dma((2,)),
            dma(()), dma(()), dma(()), dma((8, 3)), dma((8,)),
            dma(()), dma((2, 4)), dma(()), dma((4, 1)), dma(()), dma((2, 4)), dma(()), dma((4, 2)),
            dma(()), dma(()), dma(()), dma(()),
        ],
        compiler_params=pltpu.CompilerParams(
            collective_id=0, has_side_effects=True, vmem_limit_bytes=58 * 1024 * 1024
        ),
        name="linear_backward",
    )(tokens, weight, grad_output)
    return pl.pallas_call(
        put,
        out_shape=tuple(jax.ShapeDtypeStruct(block.shape, BF16) for block in blocks),
        in_specs=[pl.BlockSpec(memory_space=pltpu.VMEM)] * 2,
        out_specs=(any_spec, any_spec),
        scratch_shapes=[dma((4,)), dma((4,))],
        name="put",
    )(*[pltpu.with_memory_space_constraint(block, pltpu.VMEM) for block in blocks])


def solution(mesh):
    return jax.shard_map(
        per_device,
        mesh=mesh,
        in_specs=(P(("row", "col"), "depth"), P("depth", ("col", "row")), P("row", ("col", "depth"))),
        out_specs=(P(("row", "col"), "depth"), P("depth", ("col", "row"))),
        check_vma=False,
    )
```
